32 devices in a mesh: groups: 2 (over x), tm: 8 (over z, y), sector: 2 (over core).
Axes of the slice: x: 2, y: 2, z: 4, core: 2. Of those that a mesh axis runs over, the one named last changes fastest.
Arguments:
- context: bfloat16 [16, 2, 512, 256], P(('groups', 'tm'), 'sector'), parts along dimension 0, may hold values from -6 to 6
- depth_weight: float32 [16, 2, 16, 512], P(('groups', 'tm'), 'sector'), parts along dimension 0, may hold values from 0 to 1
- cell_ids: int32 [2, 16, 512], P('sector'), may hold values from 0 to 4095
- time_embed: bfloat16 [8, 256], replicated, may hold values from -3 to 3
- norm_gain: float32 [2, 2, 256], replicated, may hold values from 0.1 to 1.9
- w_qkv: bfloat16 [2, 256, 768], replicated, may hold values from -15 to 15
- w_out: bfloat16 [2, 256, 256], replicated, may hold values from -0.375 to 0.375
- w_up: bfloat16 [2, 256, 1024], replicated, may hold values from -0.375 to 0.375
- w_down: bfloat16 [2, 1024, 256], replicated, may hold values from -0.1875 to 0.1875
- conv_weight: bfloat16 [3, 3, 256, 256], replicated, may hold values from -0.125 to 0.125
Outputs:
- bev_out: bfloat16 [16, 64, 64, 256], P(('groups', 'tm'), 'sector'), parts along dimension 0
The draws below stay inside these ranges and needn't reach their ends.
There are 2 independent parts, one for each index of `groups`. The reference program is written for one: setup_inputs(seed, part) draws one part's arguments, and reference() takes and returns one part's arrays. A program takes and returns all parts, laid end to end along the dimension named above; an argument that names none is the same for every part. Nothing has to cross between parts.
All inputs are finite; a program needn't handle non-finite values.
Results may differ from the reference program's by a relative error of at most 0.0079.
Values may be sent and summed in bfloat16 or wider, within the bound.
No kernel may reach another device: no remote copies, remote signals or barrier semaphores. Data moves between devices by JAX's collectives and lax.ppermute only.
A program may use at most 128 MiB of HBM per device.

```python
import jax
import jax.numpy as jnp
from jax import lax

C = 256
HEADS = 8
MLP = 1024
GRID = 64
PIX = 512
DB = 16
LAYERS = 2
FRAMES = 8
SECTORS = 2


def draw_w_qkv(key, part):
    first = jax.random.fold_in(jax.random.fold_in(key, 11), 0)
    base = jnp.clip(jax.random.normal(first, (LAYERS, C, 3 * C), jnp.float32), -6.0, 6.0) * C ** (-0.5)
    return base.astype(jnp.bfloat16)


def touch_ends(result, own_key, least, top_value):
    dims = result.shape
    index_at = [jax.random.randint(jax.random.fold_in(own_key, axis), (), 0, dims[axis]) for axis in range(len(dims))]
    result = result.at[tuple(index_at)].set(least)
    longest = dims.index(max(dims))
    index_at[longest] = (index_at[longest] + 1) % dims[longest]
    return result.at[tuple(index_at)].set(top_value)


def block_levels(key, dims, cuts, least, high):
    factor_of, own = 1.0, jax.random.fold_in(key, 6)
    for dim, shards_of in cuts:
        steps = jnp.exp(jax.random.uniform(jax.random.fold_in(own, dim), (shards_of,), jnp.float32, least / len(cuts), high / len(cuts)))
        factor_of = factor_of * jnp.repeat(steps, dims[dim] // shards_of).reshape([-1 if axis == dim else 1 for axis in range(len(dims))])
    return factor_of


def normal_values(rng, extent, spread, most, shards=(), kind=jnp.bfloat16):
    factor_of = block_levels(rng, extent, shards, -0.22, 0.18) if shards else 1.0
    values = jax.random.normal(rng, extent, jnp.float32) * spread * factor_of
    return jnp.minimum(jnp.maximum(values, -most), most).astype(kind)


def setup_inputs(seed: int = 0, part: int = 0) -> dict:
    key_list = jax.random.split(jax.random.key(seed), 11)
    part_splits = jax.random.split(jax.random.fold_in(key_list[10], part), 11)
    return {
        "context": normal_values(part_splits[0], (FRAMES, SECTORS, PIX, C), 1.0, 6.0, ((0, 8), (1, 2))),
        "depth_weight": jnp.clip(1.0 * jax.random.uniform(part_splits[1], (FRAMES, SECTORS, DB, PIX), jnp.float32) ** block_levels(part_splits[1], (FRAMES, SECTORS, DB, PIX), ((0, 8), (1, 2)), -0.2, 0.2), 0.0, 1.0),
        "cell_ids": touch_ends(jax.random.randint(key_list[2], (SECTORS, DB, PIX), 0, GRID * GRID), jax.random.fold_in(key_list[2], 1), 0, (GRID * GRID) - 1).astype(jnp.int32),
        "time_embed": normal_values(key_list[3], (FRAMES, C), 0.5, 3.0),
        "norm_gain": jnp.clip(1.0 + 0.18 * jax.random.normal(key_list[4], (LAYERS, 2, C), jnp.float32), 0.1, 1.9),
        "w_qkv": draw_w_qkv(jax.random.fold_in(key_list[10], 71), part),
        "w_out": normal_values(key_list[6], (LAYERS, C, C), C ** -0.5, 0.375),
        "w_up": normal_values(key_list[7], (LAYERS, C, MLP), C ** -0.5, 0.375),
        "w_down": normal_values(key_list[8], (LAYERS, MLP, C), MLP ** -0.5, 0.1875),
        "conv_weight": normal_values(key_list[9], (3, 3, C, C), (9 * C) ** -0.5, 0.125),
    }


def pool_frame(context_frame, weight_frame, cell_ids):
    cell_count = GRID * GRID
    block_cells = min(512, cell_count)

    def one_sector(sector_inputs):
        features, weights, cell_index = sector_inputs

        def one_block(first_cell):
            target = first_cell + lax.broadcasted_iota(jnp.int32, (block_cells, 1), 0)
            matches = cell_index[:, None, :] == target[None]
            matrix = lax.optimization_barrier(jnp.sum(jnp.where(matches, weights[:, None, :], jnp.zeros_like(weights[:, None, :])), axis=0)).astype(jnp.bfloat16)
            return jnp.dot(matrix, features, preferred_element_type=jnp.float32).astype(jnp.bfloat16)
        starts = (jnp.arange(cell_count // block_cells) * block_cells).astype(jnp.int32)
        return lax.map(one_block, starts).reshape(cell_count, features.shape[-1])
    partials = lax.map(one_sector, (context_frame, weight_frame, cell_ids))
    return lax.optimization_barrier(jnp.sum(partials.astype(jnp.float32), axis=0)).astype(jnp.bfloat16)

def normalize(values, gain):
    return values * lax.rsqrt(lax.optimization_barrier(jnp.mean(values * values, axis=-1, keepdims=True)) + 1e-05) * gain

def encode_stack(tokens, time_embed, norm_gain, w_qkv, w_out, w_up, w_down):
    frame_count, cell_count, channels = tokens.shape
    head_size = channels // HEADS
    query_frame = lax.broadcasted_iota(jnp.int32, (frame_count, frame_count), 0)
    key_frame = lax.broadcasted_iota(jnp.int32, (frame_count, frame_count), 1)
    allowed = key_frame <= query_frame
    stream = (tokens.astype(jnp.float32) + time_embed[:, None, :].astype(jnp.float32)).reshape(frame_count * cell_count, channels)
    for number in range(LAYERS):
        normed = normalize(stream, norm_gain[number, 0]).astype(jnp.bfloat16)
        projected = jnp.dot(normed, w_qkv[number], preferred_element_type=jnp.float32).astype(jnp.bfloat16)
        projected = projected.reshape(frame_count, cell_count, 3, HEADS, head_size).astype(jnp.float32)
        scores = jnp.einsum('fchd,gchd->chfg', projected[:, :, 0], projected[:, :, 1]) * head_size ** (-0.5)
        scores = jnp.where(allowed, scores, -1e+30)
        largest = lax.optimization_barrier(jnp.max(scores, axis=-1, keepdims=True))
        raised = jnp.exp(scores - largest)
        soft_weights = (raised / lax.optimization_barrier(jnp.sum(raised, axis=-1, keepdims=True))).astype(jnp.bfloat16)
        mixed = jnp.einsum('chfg,gchd->fchd', soft_weights.astype(jnp.float32), projected[:, :, 2]).astype(jnp.bfloat16)
        mixed = mixed.reshape(frame_count * cell_count, channels)
        stream = stream + jnp.dot(mixed, w_out[number], preferred_element_type=jnp.float32)
        normed_second = normalize(stream, norm_gain[number, 1]).astype(jnp.bfloat16)
        hidden_units = jax.nn.gelu(jnp.dot(normed_second, w_up[number], preferred_element_type=jnp.float32), approximate=True).astype(jnp.bfloat16)
        stream = stream + jnp.dot(hidden_units, w_down[number], preferred_element_type=jnp.float32)
    return stream.reshape(frame_count, cell_count, channels).astype(jnp.bfloat16)

def convolve(frame_grid, conv_weight):
    padded = jnp.pad(frame_grid, ((1, 1), (1, 1), (0, 0)))
    summed = frame_grid.astype(jnp.float32)
    for offset in range(3):
        row_strip = padded[offset:offset + GRID]
        stacked = jnp.concatenate([row_strip[:, column:column + GRID] for column in range(3)], axis=-1)
        product = jnp.dot(stacked.reshape(GRID * GRID, 3 * C), conv_weight[offset].reshape(3 * C, C), preferred_element_type=jnp.float32)
        summed = summed + product.reshape(GRID, GRID, C)
    return summed.astype(jnp.bfloat16)

def reference(context, depth_weight, cell_ids, time_embed, norm_gain, w_qkv, w_out, w_up, w_down, conv_weight):

    def pool_one(frame_inputs):
        return pool_frame(frame_inputs[0], frame_inputs[1], cell_ids)
    pooled = lax.map(pool_one, (context, depth_weight))
    cell_count = GRID * GRID
    block_cells = min(256, cell_count)
    grouped = pooled.reshape(FRAMES, cell_count // block_cells, block_cells, C).transpose(1, 0, 2, 3)

    def encode_one(cell_group):
        return encode_stack(cell_group, time_embed, norm_gain, w_qkv, w_out, w_up, w_down)
    encoded = lax.map(encode_one, grouped)
    encoded = encoded.transpose(1, 0, 2, 3).reshape(FRAMES, GRID, GRID, C)

    def convolve_one(frame_grid):
        return convolve(frame_grid, conv_weight)
    return lax.map(convolve_one, encoded)
```

```python
import functools

import jax
import jax.numpy as jnp
from jax import lax
from jax.experimental import pallas as pl
from jax.experimental.pallas import tpu as pltpu
from jax.sharding import PartitionSpec as P

HEADS = 8
GRID = 64
LANES = 128
PACKED = 16
F32 = jnp.float32
BF16 = jnp.bfloat16
NT = (((1,), (1,)), ((), ()))


def padded_2(cells, sides, width):
    for axis, dim in sides:
        count = lax.axis_size(axis)
        ends = count - 1
        head = lax.slice_in_dim(cells, 0, width, axis=dim)
        tail = lax.slice_in_dim(cells, cells.shape[dim] - width, cells.shape[dim], axis=dim)
        cells = jnp.concatenate(
            [
                lax.ppermute(tail, axis, [(i, (i + 1) % count) for i in range(ends)]),
                cells,
                lax.ppermute(head, axis, [((i + 1) % count, i) for i in range(ends)]),
            ],
            axis=dim,
        )
    return cells


def pool_kernel(first_row, *refs):
    *sector_refs, out_ref, context_t, col_hot, row_id, matrix = refs
    sectors = len(sector_refs) // 3
    piece = pl.program_id(0)
    bins, pixels = sector_refs[1].shape
    rows = out_ref.shape[2] // GRID

    @pl.when(piece == 0)
    def _():
        for s in range(sectors):
            context, weight, ids = sector_refs[3 * s : 3 * s + 3]
            context_t[s] = context[...].astype(F32).T.astype(BF16)
            column = lax.broadcasted_iota(jnp.int32, (GRID, pixels), 0)
            for d in range(bins):
                cell = ids[d : d + 1, :]
                row = lax.div(cell, GRID)
                row_id[s, d] = jnp.broadcast_to(row.astype(F32), (PACKED, pixels)).astype(BF16)
                col_hot[s, d] = jnp.where(
                    column == cell - row * GRID, weight[d : d + 1, :], 0.0
                ).astype(BF16)

    for i in range(rows):
        target = (first_row[0] + piece * rows + i).astype(F32)
        target = jnp.full((PACKED, LANES), target, F32).astype(BF16)
        for s in range(sectors):
            for lane in range(0, pixels, LANES):
                at = slice(lane, lane + LANES)
                sums = [jnp.zeros((PACKED, LANES), BF16)] * (GRID // PACKED)
                for d in range(bins):
                    hit = row_id[s, d, :, at] == target
                    for j in range(GRID // PACKED):
                        part = col_hot[s, d, j * PACKED : (j + 1) * PACKED, at]
                        sums[j] = sums[j] + jnp.where(hit, part, jnp.zeros_like(part))
                for j in range(GRID // PACKED):
                    low = i * GRID + j * PACKED
                    matrix[s, low : low + PACKED, at] = sums[j]
    total = None
    for s in range(sectors):
        part = lax.dot_general(context_t[s], matrix[s], NT, preferred_element_type=F32)
        part = part.astype(BF16).astype(F32)
        total = part if total is None else total + part
    out_ref[0] = total.astype(BF16)


def pool(first_row, sector_args, pieces, piece_cells):
    pixels, channels = sector_args[0][0].shape
    bins = sector_args[0][1].shape[0]
    sectors = len(sector_args)
    whole = [pl.BlockSpec(memory_space=pltpu.VMEM)] * (3 * sectors)
    return pl.pallas_call(
        pool_kernel,
        grid=(pieces,),
        out_shape=jax.ShapeDtypeStruct((pieces, channels, piece_cells), BF16),
        in_specs=[pl.BlockSpec(memory_space=pltpu.SMEM)] + whole,
        out_specs=pl.BlockSpec((1, channels, piece_cells), lambda i: (i, 0, 0)),
        scratch_shapes=[
            pltpu.VMEM((sectors, channels, pixels), BF16),
            pltpu.VMEM((sectors, bins, GRID, pixels), BF16),
            pltpu.VMEM((sectors, bins, PACKED, pixels), BF16),
            pltpu.VMEM((sectors, piece_cells, pixels), BF16),
        ],
        compiler_params=pltpu.CompilerParams(dimension_semantics=("arbitrary",)),
        cost_estimate=pl.CostEstimate(
            flops=2 * sectors * pieces * piece_cells * pixels * channels,
            bytes_accessed=2 * pieces * piece_cells * channels,
            transcendentals=0,
        ),
        name="pool",
    )(first_row, *[a for args in sector_args for a in args])


def prep_kernel(w_qkv, w_out, w_up, w_down, qkv_t, out_t, up_t, down_t):
    layers, channels, _ = w_qkv.shape
    hidden = w_up.shape[2]
    size = channels // HEADS
    row = lax.broadcasted_iota(jnp.int32, (channels, channels), 0)
    col = lax.broadcasted_iota(jnp.int32, (channels, channels), 1)
    order = (col == (row % HEADS) * size + row // HEADS).astype(F32).astype(BF16)
    same = (col == row).astype(F32).astype(BF16)

    def turned(left, right):
        return lax.dot_general(left, right, NT, preferred_element_type=F32).astype(BF16)

    for l in range(layers):
        for j in range(3):
            at = slice(j * channels, (j + 1) * channels)
            qkv_t[l, at, :] = turned(order, w_qkv[l, :, at])
        rows = jnp.dot(order, w_out[l], preferred_element_type=F32).astype(BF16)
        out_t[l] = turned(same, rows)
        for j in range(0, hidden, channels):
            at = slice(j, j + channels)
            up_t[l, at, :] = turned(same, w_up[l, :, at])
            down_t[l, :, at] = turned(same, w_down[l, at, :])


def prep(w_qkv, w_out, w_up, w_down):
    turned = lambda w: jax.ShapeDtypeStruct((w.shape[0], w.shape[2], w.shape[1]), w.dtype)
    return pl.pallas_call(
        prep_kernel,
        out_shape=[turned(w) for w in (w_qkv, w_out, w_up, w_down)],
        in_specs=[pl.BlockSpec(memory_space=pltpu.VMEM)] * 4,
        out_specs=[pl.BlockSpec(memory_space=pltpu.VMEM)] * 4,
        name="prep",
    )(w_qkv, w_out, w_up, w_down)


def normed_tile(stream, gain):
    mean = jnp.mean(stream * stream, axis=0, keepdims=True)
    scale = lax.rsqrt(mean + 1e-05)
    lanes = stream.shape[1]
    gains = jnp.concatenate([gain] * (lanes // LANES), axis=1)
    return (stream * scale * gains).astype(BF16)


def query_groups(frames, most):
    groups, group, pairs = [], [], 0
    for f in range(frames):
        if group and pairs + f + 1 > most:
            groups.append(group)
            group, pairs = [], 0
        group.append(f)
        pairs += f + 1
    return groups + [group]


def attention(qkv, mixed, frames, cells, channels):
    size = channels // HEADS
    for group in query_groups(frames, 40):
        last = group[-1]
        for lane in range(0, cells, LANES):
            pairs = [(f, g) for f in group for g in range(f + 1)]

            def at(f):
                return slice(f * cells + lane, f * cells + lane + LANES)

            def score_step(d, sums):
                row = pl.multiple_of(d * HEADS, HEADS)
                query = {f: qkv[pl.ds(row, HEADS), at(f)] for f in group}
                keys = [qkv[pl.ds(channels + row, HEADS), at(g)] for g in range(last + 1)]
                return tuple(s + query[f] * keys[g] for s, (f, g) in zip(sums, pairs))

            zeros = tuple(jnp.zeros((HEADS, LANES), F32) for _ in pairs)
            scores = dict(zip(pairs, lax.fori_loop(0, size, score_step, zeros, unroll=4)))
            weights = {}
            for f in group:
                row = [scores[f, g] for g in range(f + 1)]
                largest = functools.reduce(jnp.maximum, row)
                raised = [jnp.exp((s - largest) * size ** (-0.5)) for s in row]
                share = 1.0 / functools.reduce(jnp.add, raised)
                for g in range(f + 1):
                    weights[f, g] = (raised[g] * share).astype(BF16).astype(F32)

            def mix_step(step, carry):
                parts = {f: [] for f in group}
                for half in range(2):
                    row = pl.multiple_of(2 * channels + (2 * step + half) * HEADS, HEADS)
                    values = [qkv[pl.ds(row, HEADS), at(g)] for g in range(last + 1)]
                    for f in group:
                        terms = [carry[pairs.index((f, g))] * values[g] for g in range(f + 1)]
                        parts[f].append(functools.reduce(jnp.add, terms))
                low = pl.multiple_of(step * 2 * HEADS, 2 * HEADS)
                for f in group:
                    mixed[pl.ds(low, 2 * HEADS), at(f)] = jnp.concatenate(
                        parts[f], axis=0
                    ).astype(BF16)
                return carry

            lax.fori_loop(
                0, size // 2, mix_step, tuple(weights[pair] for pair in pairs), unroll=2
            )


def encode_kernel(
    tokens, embed, gains, qkv_t, out_t, up_t, down_t, encoded, stream, qkv, mixed, *, tile
):
    frames, channels, cells = tokens.shape
    layers = qkv_t.shape[0]
    lanes = frames * cells
    for f in range(frames):
        for lane in range(0, cells, LANES):
            stream[:, f * cells + lane : f * cells + lane + LANES] = (
                tokens[f, :, lane : lane + LANES].astype(F32) + embed[f]
            )

    def layer(l, _):
        def project(t, _):
            at = pl.ds(pl.multiple_of(t * tile, tile), tile)
            normed = normed_tile(stream[:, at], gains[l, 0])
            out = jnp.dot(qkv_t[l], normed, preferred_element_type=F32)
            qkv[:, at] = out.astype(BF16).astype(F32)
            return 0

        lax.fori_loop(0, lanes // tile, project, 0)
        attention(qkv, mixed, frames, cells, channels)

        def feed(t, _):
            at = pl.ds(pl.multiple_of(t * tile, tile), tile)
            current = stream[:, at] + jnp.dot(
                out_t[l], mixed[:, at], preferred_element_type=F32
            )
            normed = normed_tile(current, gains[l, 1])
            up = jnp.dot(up_t[l], normed, preferred_element_type=F32)
            hidden = jax.nn.gelu(up, approximate=True).astype(BF16)
            stream[:, at] = current + jnp.dot(down_t[l], hidden, preferred_element_type=F32)
            return 0

        lax.fori_loop(0, lanes // tile, feed, 0)
        return 0

    lax.fori_loop(0, layers, layer, 0)
    for f in range(frames):
        encoded[f] = stream[:, f * cells : (f + 1) * cells].T.astype(BF16)


def encode(tokens, embed, gains, weights):
    frames, channels, cells = tokens.shape
    layers, hidden = weights[2].shape[:2]
    lanes = frames * cells
    tile = min(lanes, 512)
    count = frames * cells
    return pl.pallas_call(
        functools.partial(encode_kernel, tile=tile),
        out_shape=jax.ShapeDtypeStruct((frames, cells, channels), BF16),
        in_specs=[pl.BlockSpec(memory_space=pltpu.VMEM)] * 7,
        out_specs=pl.BlockSpec(memory_space=pltpu.VMEM),
        scratch_shapes=[
            pltpu.VMEM((channels, lanes), F32),
            pltpu.VMEM((3 * channels, lanes), F32),
            pltpu.VMEM((channels, lanes), BF16),
        ],
        cost_estimate=pl.CostEstimate(
            flops=2 * layers * count * channels * (4 * channels + 2 * hidden),
            bytes_accessed=4 * count * channels,
            transcendentals=layers * count * hidden,
        ),
        name="encode",
    )(tokens, embed, gains, *weights)


def body(
    context, depth_weight, cell_ids, time_embed, norm_gain, w_qkv, w_out, w_up, w_down, conv_weight
):
    sector_count = lax.axis_size("sector")
    tm_count = lax.axis_size("tm")
    frames_dev, _, _, channels = context.shape
    band_cells = GRID * GRID // sector_count
    piece_cells = band_cells // tm_count
    row_count = band_cells // GRID

    def from_others(value):
        values = [value]
        for shift in range(1, sector_count):
            ring = [(i, (i + shift) % sector_count) for i in range(sector_count)]
            values.append(lax.ppermute(value, "sector", ring))
        return values

    contexts, depths, ids = map(from_others, (context[:, 0], depth_weight[:, 0], cell_ids[0]))
    first_row = (lax.axis_index("sector") * row_count).astype(jnp.int32).reshape(1)
    weights = prep(w_qkv, w_out, w_up, w_down)
    embed = jnp.broadcast_to(time_embed.astype(F32)[:, :, None], time_embed.shape + (LANES,))
    gains = jnp.broadcast_to(norm_gain[..., None], norm_gain.shape + (LANES,))
    pooled = jnp.stack(
        [
            pool(
                first_row,
                [(c[n], w[n], i) for c, w, i in zip(contexts, depths, ids)],
                tm_count,
                piece_cells,
            )
            for n in range(frames_dev)
        ]
    )
    received = lax.all_to_all(pooled, "tm", split_axis=1, concat_axis=0, tiled=True)
    tokens = received.reshape(frames_dev * tm_count, channels, piece_cells)
    spare = -piece_cells % LANES
    tokens = jnp.pad(tokens, ((0, 0), (0, 0), (0, spare)))
    encoded = encode(tokens, embed, gains, weights)[:, :piece_cells]
    encoded = encoded.reshape(tm_count, frames_dev, piece_cells, channels)
    encoded = encoded.transpose(1, 0, 2, 3)
    returned = lax.all_to_all(encoded, "tm", split_axis=1, concat_axis=0, tiled=True)
    returned = returned.reshape(tm_count, frames_dev, piece_cells, channels).transpose(1, 0, 2, 3)
    encoded = returned.reshape(frames_dev, row_count, GRID, channels)
    padded = padded_2(encoded, (("sector", 1),), 1)
    padded = jnp.pad(padded, ((0, 0), (0, 0), (1, 1), (0, 0)))
    summed = encoded.astype(F32)
    for offset in range(3):
        row_strip = padded[:, offset : offset + row_count]
        stacked = jnp.concatenate(
            [row_strip[:, :, column : column + GRID] for column in range(3)], axis=-1
        )
        product = jnp.dot(
            stacked.reshape(frames_dev * row_count * GRID, 3 * channels),
            conv_weight[offset].reshape(3 * channels, channels),
            preferred_element_type=F32,
        )
        summed = summed + product.reshape(summed.shape)
    return summed.astype(BF16)


def solution(mesh):
    return jax.shard_map(
        body,
        mesh=mesh,
        in_specs=(
            P(("groups", "tm"), "sector", None, None),
            P(("groups", "tm"), "sector", None, None),
            P("sector", None, None),
            P(),
            P(),
            P(),
            P(),
            P(),
            P(),
            P(),
        ),
        out_specs=P(("groups", "tm"), "sector", None, None),
        check_vma=False,
    )
```

```python
import functools
import math

import jax
import jax.numpy as jnp
from jax import lax
from jax.experimental import pallas as pl
from jax.experimental.pallas import tpu as pltpu
from jax.sharding import PartitionSpec as P

HEADS = 8
GRID = 64
LANES = 128
TILE_LANES = 256
SUBLANES = 8
VMEM_LIMIT = 24 << 20
F32 = jnp.float32
BF16 = jnp.bfloat16
NT = (((1,), (1,)), ((), ()))


def pool_kernel(place, *refs, slots, piece_rows, chunk_order):
    *sector_refs, context_t, col_hot, row_id, matrix = refs
    out_refs = sector_refs[-len(slots) :]
    sector_refs = sector_refs[: -len(slots)]
    sectors = len(sector_refs) // 3
    bins, pixels = sector_refs[1].shape
    blocks = pixels // TILE_LANES
    shape = (SUBLANES, TILE_LANES)
    wide = (SUBLANES, pixels)

    column = lax.broadcasted_iota(jnp.int32, wide, 0).astype(F32).astype(BF16)
    for s in range(sectors):
        context, weight, ids = sector_refs[3 * s : 3 * s + 3]
        context_t[s] = context[...].astype(F32).T.astype(BF16)
        rows = lax.div(ids[...], GRID)
        cols = (ids[...] - rows * GRID).astype(F32)
        rows = rows.astype(F32)
        for d in range(bins):
            row_id[s, d] = jnp.broadcast_to(rows[d : d + 1], wide).astype(BF16)
            col = jnp.broadcast_to(cols[d : d + 1], wide).astype(BF16)
            value = jnp.broadcast_to(weight[d : d + 1, :], wide).astype(BF16)
            for j in range(GRID // SUBLANES):
                low = j * SUBLANES
                hit = column + low == col
                col_hot[s, d, low : low + SUBLANES] = jnp.where(
                    hit, value, jnp.zeros_like(value)
                )

    for slot, out_ref in zip(slots, out_refs):
        piece = place[0] ^ slot
        for first in range(0, piece_rows, 2):
            targets = []
            for row in chunk_order[first : first + 2]:
                target = (place[1] + piece * piece_rows + row).astype(F32)
                targets.append(jnp.full(shape, target, F32).astype(BF16))

            def match(n, _):
                s = n // blocks
                at = pl.ds(pl.multiple_of((n % blocks) * TILE_LANES, TILE_LANES), TILE_LANES)
                sums = [[jnp.zeros(shape, BF16)] * (GRID // SUBLANES) for _ in targets]
                for d in range(bins):
                    row = row_id[s, d, :, at]
                    hits = [row == target for target in targets]
                    for j in range(GRID // SUBLANES):
                        part = col_hot[s, d, j * SUBLANES : (j + 1) * SUBLANES, at]
                        for k, hit in enumerate(hits):
                            sums[k][j] = sums[k][j] + jnp.where(hit, part, jnp.zeros_like(part))
                for k in range(len(targets)):
                    for j in range(GRID // SUBLANES):
                        low = (first + k) * GRID + j * SUBLANES
                        matrix[s, low : low + SUBLANES, at] = sums[k][j]
                return 0

            lax.fori_loop(0, sectors * blocks, match, 0)
        total = None
        for s in range(sectors):
            part = lax.dot_general(context_t[s], matrix[s], NT, preferred_element_type=F32)
            part = part.astype(BF16).astype(F32)
            total = part if total is None else total + part
        out_ref[...] = total.astype(BF16)


def pool(place, sector_args, slots, piece_rows, chunk_order):
    pixels, channels = sector_args[0][0].shape
    bins = sector_args[0][1].shape[0]
    sectors = len(sector_args)
    cells = piece_rows * GRID
    vmem = pl.BlockSpec(memory_space=pltpu.VMEM)
    return pl.pallas_call(
        functools.partial(
            pool_kernel, slots=slots, piece_rows=piece_rows, chunk_order=chunk_order
        ),
        out_shape=[jax.ShapeDtypeStruct((channels, cells), BF16)] * len(slots),
        in_specs=[pl.BlockSpec(memory_space=pltpu.SMEM)] + [vmem] * (3 * sectors),
        out_specs=[vmem] * len(slots),
        scratch_shapes=[
            pltpu.VMEM((sectors, channels, pixels), BF16),
            pltpu.VMEM((sectors, bins, GRID, pixels), BF16),
            pltpu.VMEM((sectors, bins, SUBLANES, pixels), BF16),
            pltpu.VMEM((sectors, cells, pixels), BF16),
        ],
        compiler_params=pltpu.CompilerParams(vmem_limit_bytes=VMEM_LIMIT),
        cost_estimate=pl.CostEstimate(
            flops=2 * sectors * len(slots) * cells * pixels * channels,
            bytes_accessed=2 * len(slots) * cells * channels,
            transcendentals=0,
        ),
        name="pool",
    )(place, *[a for args in sector_args for a in args])


def prep_kernel(w_qkv, w_out, w_up, w_down, gain, embed, qkv_t, out_t, up_t, down_t, gains, embeds):
    _, channels, _ = w_qkv.shape
    hidden = w_up.shape[2]
    size = channels // HEADS
    row = lax.broadcasted_iota(jnp.int32, (channels, channels), 0)
    col = lax.broadcasted_iota(jnp.int32, (channels, channels), 1)
    order = (col == (row % HEADS) * size + row // HEADS).astype(F32).astype(BF16)
    same = (col == row).astype(F32).astype(BF16)

    def turned(left, right):
        return lax.dot_general(left, right, NT, preferred_element_type=F32).astype(BF16)

    def columns(values):
        return jnp.broadcast_to(values, (LANES, channels)).T

    for j in range(3):
        at = slice(j * channels, (j + 1) * channels)
        qkv_t[0, at, :] = turned(order, w_qkv[0, :, at])
    rows = jnp.dot(order, w_out[0], preferred_element_type=F32).astype(BF16)
    out_t[0] = turned(same, rows)
    for j in range(0, hidden, channels):
        at = slice(j, j + channels)
        up_t[0, at, :] = turned(same, w_up[0, :, at])
        down_t[0, :, at] = turned(same, w_down[0, at, :])
    for k in range(gain.shape[1]):
        gains[0, k] = columns(gain[0, k : k + 1, :])

    @pl.when(pl.program_id(0) == 0)
    def _():
        for f in range(embed.shape[0]):
            embeds[f] = columns(embed[f : f + 1, :].astype(F32))


def prep(w_qkv, w_out, w_up, w_down, norm_gain, time_embed):
    matrices = (w_qkv, w_out, w_up, w_down)
    channels = time_embed.shape[1]
    a_layer = lambda shape: pl.BlockSpec((1,) + shape[1:], lambda l: (l,) + (0,) * (len(shape) - 1))
    whole = lambda shape: pl.BlockSpec(shape, lambda l: (0,) * len(shape))
    gains = norm_gain.shape + (LANES,)
    embeds = time_embed.shape + (LANES,)
    turned = [(w.shape[0], w.shape[2], w.shape[1]) for w in matrices]
    return pl.pallas_call(
        prep_kernel,
        grid=(w_qkv.shape[0],),
        out_shape=[jax.ShapeDtypeStruct(shape, BF16) for shape in turned]
        + [jax.ShapeDtypeStruct(gains, F32), jax.ShapeDtypeStruct(embeds, F32)],
        in_specs=[a_layer(w.shape) for w in matrices]
        + [a_layer(norm_gain.shape), whole(time_embed.shape)],
        out_specs=[a_layer(shape) for shape in turned] + [a_layer(gains), whole(embeds)],
        compiler_params=pltpu.CompilerParams(
            dimension_semantics=("arbitrary",), vmem_limit_bytes=VMEM_LIMIT
        ),
        cost_estimate=pl.CostEstimate(
            flops=2 * channels * sum(w.size for w in matrices),
            bytes_accessed=4 * sum(w.size for w in matrices),
            transcendentals=0,
        ),
        name="prep",
    )(*matrices, norm_gain, time_embed)


def normed_tile(stream, gain):
    mean = jnp.mean(stream * stream, axis=0, keepdims=True)
    scale = lax.rsqrt(mean + 1e-05)
    lanes = stream.shape[1]
    gains = jnp.concatenate([gain] * (lanes // LANES), axis=1)
    return (stream * scale * gains).astype(BF16)


def gelu(values):
    root = (2.0 / math.pi) ** 0.5
    half = 0.5 * values
    return half + half * jnp.tanh(values * (root + (root * 0.044715) * (values * values)))


def query_groups(frames, most):
    groups, group, pairs = [], [], 0
    for f in range(frames):
        if group and pairs + f + 1 > most:
            groups.append(group)
            group, pairs = [], 0
        group.append(f)
        pairs += f + 1
    return groups + [group]


def attention(qkv, mixed, frames, cells, channels):
    size = channels // HEADS
    for group in query_groups(frames, 40):
        last = group[-1]
        for lane in range(0, cells, LANES):
            pairs = [(f, g) for f in group for g in range(f + 1)]

            def at(f):
                return slice(f * cells + lane, f * cells + lane + LANES)

            def score_step(d, sums):
                row = pl.multiple_of(d * HEADS, HEADS)
                query = {f: qkv[pl.ds(row, HEADS), at(f)] for f in group}
                keys = [qkv[pl.ds(channels + row, HEADS), at(g)] for g in range(last + 1)]
                return tuple(s + query[f] * keys[g] for s, (f, g) in zip(sums, pairs))

            zeros = tuple(jnp.zeros((HEADS, LANES), F32) for _ in pairs)
            scores = dict(zip(pairs, lax.fori_loop(0, size, score_step, zeros, unroll=4)))
            weights = {}
            for f in group:
                row = [scores[f, g] for g in range(f + 1)]
                largest = functools.reduce(jnp.maximum, row)
                raised = [jnp.exp((s - largest) * size ** (-0.5)) for s in row]
                share = 1.0 / functools.reduce(jnp.add, raised)
                for g in range(f + 1):
                    weights[f, g] = (raised[g] * share).astype(BF16).astype(F32)

            def mix_step(step, carry):
                parts = {f: [] for f in group}
                for half in range(2):
                    row = pl.multiple_of(2 * channels + (2 * step + half) * HEADS, HEADS)
                    values = [qkv[pl.ds(row, HEADS), at(g)] for g in range(last + 1)]
                    for f in group:
                        terms = [carry[pairs.index((f, g))] * values[g] for g in range(f + 1)]
                        parts[f].append(functools.reduce(jnp.add, terms))
                low = pl.multiple_of(step * 2 * HEADS, 2 * HEADS)
                for f in group:
                    mixed[pl.ds(low, 2 * HEADS), at(f)] = jnp.concatenate(
                        parts[f], axis=0
                    ).astype(BF16)
                return carry

            lax.fori_loop(
                0, size // 2, mix_step, tuple(weights[pair] for pair in pairs), unroll=2
            )


def encode_kernel(place, *refs, slots, chunk, cells, valid, last, tile):
    *refs, stream, qkv, mixed = refs
    tokens, refs = refs[:slots], refs[slots:]
    embed, gains, qkv_t, out_t, up_t, down_t, *outs = refs
    half = slots // 2
    layers, _, channels = qkv_t.shape
    lanes = slots * cells
    for k in range(slots):
        frame = place[0] ^ k
        for lane in range(0, cells, LANES):
            at = pl.ds(pl.multiple_of(frame * cells + lane, LANES), LANES)
            low = chunk * cells + lane
            stream[:, at] = tokens[k][:, low : low + LANES].astype(F32) + embed[frame]

    def layer(l, _):
        def project(t, _):
            at = pl.ds(pl.multiple_of(t * tile, tile), tile)
            normed = normed_tile(stream[:, at], gains[l, 0])
            out = jnp.dot(qkv_t[l], normed, preferred_element_type=F32)
            qkv[:, at] = out.astype(BF16).astype(F32)
            return 0

        lax.fori_loop(0, lanes // tile, project, 0)
        attention(qkv, mixed, slots, cells, channels)

        def feed(t, _):
            at = pl.ds(pl.multiple_of(t * tile, tile), tile)
            current = stream[:, at] + jnp.dot(
                out_t[l], mixed[:, at], preferred_element_type=F32
            )
            normed = normed_tile(current, gains[l, 1])
            up = jnp.dot(up_t[l], normed, preferred_element_type=F32)
            hidden = gelu(up).astype(BF16)
            stream[:, at] = current + jnp.dot(down_t[l], hidden, preferred_element_type=F32)
            return 0

        lax.fori_loop(0, lanes // tile, feed, 0)
        return 0

    lax.fori_loop(0, layers, layer, 0)
    earlier, outs = outs[:chunk] if last else [], outs[chunk:] if last else outs
    for k in range(slots):
        at = pl.ds(pl.multiple_of((place[0] ^ k) * cells, LANES), cells)
        done = stream[:, at].T.astype(BF16)[:valid]
        if not last:
            outs[k // half][k % half] = done
        elif k >= half:
            outs[k][...] = done
        else:
            for c, before in enumerate(earlier):
                outs[k][c * valid : (c + 1) * valid] = before[k]
            outs[k][chunk * valid : (chunk + 1) * valid] = done


def encode(place, tokens, weights, gains, embed, earlier, chunk, chunks):
    slots = len(tokens)
    half = slots // 2
    channels, piece_cells = tokens[0].shape
    valid = piece_cells // chunks
    spare = -valid % LANES
    if spare:
        tokens = [jnp.pad(t, ((0, 0), (0, spare))) for t in tokens]
    cells = valid + spare
    layers, hidden = weights[2].shape[:2]
    lanes = slots * cells
    last = chunk == chunks - 1
    if last:
        shapes = [(chunks * valid, channels)] * half + [(valid, channels)] * half
    else:
        shapes = [(half, valid, channels)] * 2
    vmem = pl.BlockSpec(memory_space=pltpu.VMEM)
    operands = [*tokens, embed, gains, *weights, *(earlier if last else [])]
    return pl.pallas_call(
        functools.partial(
            encode_kernel,
            slots=slots,
            chunk=chunk,
            cells=cells,
            valid=valid,
            last=last,
            tile=min(lanes, 512),
        ),
        out_shape=[jax.ShapeDtypeStruct(shape, BF16) for shape in shapes],
        in_specs=[pl.BlockSpec(memory_space=pltpu.SMEM)] + [vmem] * len(operands),
        out_specs=[vmem] * len(shapes),
        scratch_shapes=[
            pltpu.VMEM((channels, lanes), F32),
            pltpu.VMEM((3 * channels, lanes), F32),
            pltpu.VMEM((channels, lanes), BF16),
        ],
        compiler_params=pltpu.CompilerParams(vmem_limit_bytes=VMEM_LIMIT),
        cost_estimate=pl.CostEstimate(
            flops=2 * layers * lanes * channels * (4 * channels + 2 * hidden),
            bytes_accessed=4 * lanes * channels,
            transcendentals=layers * lanes * hidden,
        ),
        name="encode",
    )(place, *operands)


def edge_kernel(place, *refs, slots, rows, single):
    parts, outs = refs[:slots], refs[slots:]
    for k in range(slots):
        piece = place[0] ^ k
        is_head, is_tail = piece == 0, piece == slots - 1
        if single:
            is_head = jnp.logical_and(is_head, place[1] != 0)
            is_tail = jnp.logical_and(is_tail, place[1] == 0)

        @pl.when(is_head)
        def _():
            outs[0][...] = parts[k][0:GRID]

        @pl.when(is_tail)
        def _():
            outs[-1][...] = parts[k][rows - GRID : rows]


def edges(place, parts, rows, single):
    channels = parts[0].shape[1]
    vmem = pl.BlockSpec(memory_space=pltpu.VMEM)
    count = 1 if single else 2
    return pl.pallas_call(
        functools.partial(edge_kernel, slots=len(parts), rows=rows, single=single),
        out_shape=[jax.ShapeDtypeStruct((GRID, channels), BF16)] * count,
        in_specs=[pl.BlockSpec(memory_space=pltpu.SMEM)] + [vmem] * len(parts),
        out_specs=[vmem] * count,
        compiler_params=pltpu.CompilerParams(vmem_limit_bytes=VMEM_LIMIT),
        name="edges",
    )(place, *parts)


def conv_kernel(place, top, bottom, *refs, layout, chunks, piece_rows, bands, block):
    *parts, weight, out_ref, rows = refs
    slots = len(layout)
    total = slots * piece_rows
    inside = (place[1] > 0, place[1] < (bands - 1) * total)
    for edge, has, low in ((top, inside[0], 0), (bottom, inside[1], (total + 1) * GRID)):
        keep = jnp.full(edge.shape, has.astype(jnp.int32), jnp.int32) > 0
        rows[low : low + GRID] = jnp.where(keep, edge[...].astype(F32), 0.0).astype(BF16)
    for k in range(slots):
        base = (1 + (place[0] ^ k) * piece_rows) * GRID
        for c, chunk in enumerate(chunks):
            source, start = layout[k][c]
            for i, row in enumerate(chunk):
                low = pl.multiple_of(base + row * GRID, GRID)
                first = start + i * GRID
                rows[pl.ds(low, GRID)] = parts[source][first : first + GRID]

    cells = block * GRID
    column = lax.broadcasted_iota(jnp.int32, (cells, 1), 0) % GRID

    def one_block(n, _):
        def taps(j):
            sums = None
            for i in range(3):
                at = pl.ds(pl.multiple_of((n * block + i) * GRID, GRID), cells)
                product = jnp.dot(rows[at], weight[i, j], preferred_element_type=F32)
                sums = product if sums is None else sums + product
            return sums

        at = pl.ds(pl.multiple_of((n * block + 1) * GRID, GRID), cells)
        summed = rows[at].astype(F32) + taps(1)
        summed = summed + jnp.where(column == 0, 0.0, pltpu.roll(taps(0), 1, 0))
        summed = summed + jnp.where(column == GRID - 1, 0.0, pltpu.roll(taps(2), cells - 1, 0))
        out_ref[pl.ds(pl.multiple_of(n * cells, cells), cells)] = summed.astype(BF16)
        return 0

    lax.fori_loop(0, total // block, one_block, 0)


def convolve(place, top, bottom, parts, weight, layout, chunks, bands):
    channels = weight.shape[-1]
    piece_rows = sum(len(chunk) for chunk in chunks)
    total = len(layout) * piece_rows
    vmem = pl.BlockSpec(memory_space=pltpu.VMEM)
    return pl.pallas_call(
        functools.partial(
            conv_kernel,
            layout=layout,
            chunks=chunks,
            piece_rows=piece_rows,
            bands=bands,
            block=math.gcd(total, 8),
        ),
        out_shape=jax.ShapeDtypeStruct((total * GRID, channels), BF16),
        in_specs=[pl.BlockSpec(memory_space=pltpu.SMEM)] + [vmem] * (len(parts) + 3),
        out_specs=vmem,
        scratch_shapes=[pltpu.VMEM(((total + 2) * GRID, channels), BF16)],
        compiler_params=pltpu.CompilerParams(vmem_limit_bytes=VMEM_LIMIT),
        cost_estimate=pl.CostEstimate(
            flops=2 * total * GRID * weight.size,
            bytes_accessed=4 * total * GRID * channels,
            transcendentals=0,
        ),
        name="convolve",
    )(place, top, bottom, *parts, weight)


def row_chunks(piece_rows):
    if piece_rows % 4:
        return (tuple(range(piece_rows)),)
    quarter = piece_rows // 4
    inner = tuple(range(quarter, 3 * quarter))
    outer = tuple(range(quarter)) + tuple(range(3 * quarter, piece_rows))
    return (outer, inner)


def body(
    context, depth_weight, cell_ids, time_embed, norm_gain, w_qkv, w_out, w_up, w_down, conv_weight
):
    sectors = lax.axis_size("sector")
    slots = lax.axis_size("tm")
    half = slots // 2
    if context.shape[0] != 1 or slots & (slots - 1):
        raise ValueError("unsupported mesh")
    band_rows = GRID // sectors
    piece_rows = band_rows // slots
    chunks = row_chunks(piece_rows)
    valid = piece_rows * GRID // len(chunks)
    band = lax.axis_index("sector").astype(jnp.int32)
    place = jnp.stack([lax.axis_index("tm").astype(jnp.int32), band * band_rows])

    def from_others(value):
        values = [value]
        for shift in range(1, sectors):
            ring = [(i, (i + shift) % sectors) for i in range(sectors)]
            values.append(lax.ppermute(value, "sector", ring))
        return values

    def swap(value, k):
        return lax.ppermute(value, "tm", [(i, i ^ k) for i in range(slots)])

    sector_args = list(
        zip(*map(from_others, (context[0, 0], depth_weight[0, 0], cell_ids[0])))
    )
    chunk_order = sum(chunks, ())
    far, near = tuple(range(half, slots))[::-1], tuple(range(half))
    tokens = {}
    for group in (far, near):
        pooled = pool(place, sector_args, group, piece_rows, chunk_order)
        for k, value in zip(group, pooled):
            tokens[k] = swap(value, k) if k else value
    tokens = [tokens[k] for k in range(slots)]
    *weights, gains, embed = prep(w_qkv, w_out, w_up, w_down, norm_gain, time_embed)

    earlier, crossed = [], []
    for c in range(len(chunks) - 1):
        near_part, far_part = encode(place, tokens, weights, gains, embed, [], c, len(chunks))
        earlier.append(near_part)
        crossed.append(swap(far_part, half))
    outs = encode(
        place, tokens, weights, gains, embed, earlier, len(chunks) - 1, len(chunks)
    )
    parts, layout = [], [[None] * len(chunks) for _ in range(slots)]

    for k in far:
        parts.append(swap(outs[k], k))
        layout[k][-1] = (len(parts) - 1, 0)
    for k in near:
        parts.append(swap(outs[k], k) if k else outs[k])
        for c in range(len(chunks)):
            layout[k][c] = (len(parts) - 1, c * valid)
    for c, received in enumerate(crossed):
        for k in near:
            parts.append(swap(received[k], k) if k else received[k])
            layout[half + k][c] = (len(parts) - 1, 0)

    first = [parts[layout[k][0][0]] for k in range(slots)]
    up = [(i, i + 1) for i in range(sectors - 1)]
    down = [(i + 1, i) for i in range(sectors - 1)]
    if sectors == 2:
        (edge,) = edges(place, first, valid, True)
        top = bottom = lax.ppermute(edge, "sector", up + down)
    else:
        head, tail = edges(place, first, valid, False)
        top, bottom = lax.ppermute(tail, "sector", up), lax.ppermute(head, "sector", down)
    out = convolve(place, top, bottom, parts, conv_weight, layout, chunks, sectors)
    return out.reshape(1, band_rows, GRID, -1)


def solution(mesh):
    return jax.shard_map(
        body,
        mesh=mesh,
        in_specs=(
            P(("groups", "tm"), "sector", None, None),
            P(("groups", "tm"), "sector", None, None),
            P("sector", None, None),
            P(),
            P(),
            P(),
            P(),
            P(),
            P(),
            P(),
        ),
        out_specs=P(("groups", "tm"), "sector", None, None),
        check_vma=False,
    )
```

```python
import functools
import math

import jax
import jax.numpy as jnp
from jax import lax
from jax.experimental import pallas as pl
from jax.experimental.pallas import tpu as pltpu
from jax.sharding import PartitionSpec as P


HEADS = 8
GRID = 64
LANES = 128
TILE_LANES = 256
SUBLANES = 8
VMEM_LIMIT = 24 << 20
F32 = jnp.float32
BF16 = jnp.bfloat16
NT = (((1,), (1,)), ((), ()))


def mark(weights, ids, col_hot, row_id):
    bins, pixels = weights[0].shape
    wide = (SUBLANES, pixels)
    column = lax.broadcasted_iota(jnp.int32, wide, 0).astype(F32).astype(BF16)
    for s in range(len(weights)):
        rows = lax.div(ids[s][...], GRID)
        cols = (ids[s][...] - rows * GRID).astype(F32)
        rows = rows.astype(F32)
        for d in range(bins):
            row_id[s, d] = jnp.broadcast_to(rows[d : d + 1], wide).astype(BF16)
            col = jnp.broadcast_to(cols[d : d + 1], wide).astype(BF16)
            value = jnp.broadcast_to(weights[s][d : d + 1, :], wide).astype(BF16)
            for j in range(GRID // SUBLANES):
                low = j * SUBLANES
                hit = column + low == col
                col_hot[s, d, low : low + SUBLANES] = jnp.where(
                    hit, value, jnp.zeros_like(value)
                )


def match(place, slot, matrix, base, col_hot, row_id, piece_rows, chunk_order):
    sectors, bins, _, pixels = col_hot.shape
    blocks = pixels // TILE_LANES
    shape = (SUBLANES, TILE_LANES)
    piece = place[0] ^ slot
    for first in range(0, piece_rows, 2):
        targets = []
        for row in chunk_order[first : first + 2]:
            target = (place[1] + piece * piece_rows + row).astype(F32)
            targets.append(jnp.full(shape, target, F32).astype(BF16))

        def step(n, _):
            s = n // blocks
            at = pl.ds(pl.multiple_of((n % blocks) * TILE_LANES, TILE_LANES), TILE_LANES)
            sums = [[jnp.zeros(shape, BF16)] * (GRID // SUBLANES) for _ in targets]
            for d in range(bins):
                row = row_id[s, d, :, at]
                hits = [row == target for target in targets]
                for j in range(GRID // SUBLANES):
                    part = col_hot[s, d, j * SUBLANES : (j + 1) * SUBLANES, at]
                    for k, hit in enumerate(hits):
                        sums[k][j] = sums[k][j] + jnp.where(hit, part, jnp.zeros_like(part))
            for k in range(len(targets)):
                for j in range(GRID // SUBLANES):
                    low = base + (first + k) * GRID + j * SUBLANES
                    matrix[s, low : low + SUBLANES, at] = sums[k][j]
            return 0

        lax.fori_loop(0, sectors * blocks, step, 0)


def multiply(context_t, matrix, low, cells):
    total = None
    for s in range(matrix.shape[0]):
        rows = matrix[s, low : low + cells]
        part = lax.dot_general(context_t[s], rows, NT, preferred_element_type=F32)
        part = part.astype(BF16).astype(F32)
        total = part if total is None else total + part
    return total.astype(BF16)


def pool_kernel(place, *refs, slots, piece_rows, chunk_order):
    *refs, context_t, col_hot, row_id, matrix, context, weight, ids, arrived = refs
    out_refs, refs = refs[-len(slots) :], refs[: -len(slots)]
    held = (context, weight, ids)
    copies = [pltpu.make_async_copy(refs[n], held[n], arrived.at[n]) for n in range(3)]
    for copy in copies:
        copy.start()
    for copy in copies:
        copy.wait()
    refs = held + tuple(refs[3:])
    mark(refs[1::3], refs[2::3], col_hot, row_id)
    for s, context in enumerate(refs[0::3]):
        context_t[s] = context[...].astype(F32).T.astype(BF16)
    for slot, out_ref in zip(slots, out_refs):
        match(place, slot, matrix, 0, col_hot, row_id, piece_rows, chunk_order)
        out_ref[...] = multiply(context_t, matrix, 0, matrix.shape[1])


def match_kernel(place, *refs, slots, piece_rows, chunk_order):
    *refs, matrix, col_hot, row_id = refs
    mark(refs[0::2], refs[1::2], col_hot, row_id)
    cells = piece_rows * GRID
    for n, slot in enumerate(slots):
        match(place, slot, matrix, n * cells, col_hot, row_id, piece_rows, chunk_order)


def multiply_kernel(*refs, sectors):
    contexts, matrix = refs[:sectors], refs[sectors]
    out_refs, context_t = refs[sectors + 1 : -1], refs[-1]
    for s in range(sectors):
        context_t[s] = contexts[s][...].astype(F32).T.astype(BF16)
    cells = matrix.shape[1] // len(out_refs)
    for n, out_ref in enumerate(out_refs):
        out_ref[...] = multiply(context_t, matrix, n * cells, cells)


def hot_scratch(sectors, bins, pixels):
    return [
        pltpu.VMEM((sectors, bins, GRID, pixels), BF16),
        pltpu.VMEM((sectors, bins, SUBLANES, pixels), BF16),
    ]


def pool(place, contexts, depths, ids, slots, piece_rows, chunk_order):
    pixels, channels = contexts[0].shape
    bins = depths[0].shape[0]
    sectors = len(contexts)
    cells = piece_rows * GRID
    vmem = pl.BlockSpec(memory_space=pltpu.VMEM)
    return pl.pallas_call(
        functools.partial(
            pool_kernel, slots=slots, piece_rows=piece_rows, chunk_order=chunk_order
        ),
        out_shape=[jax.ShapeDtypeStruct((channels, cells), BF16)] * len(slots),
        in_specs=[pl.BlockSpec(memory_space=pltpu.SMEM)]
        + [pl.BlockSpec(memory_space=pltpu.HBM)] * 3
        + [vmem] * (3 * sectors - 3),
        out_specs=[vmem] * len(slots),
        scratch_shapes=[pltpu.VMEM((sectors, channels, pixels), BF16)]
        + hot_scratch(sectors, bins, pixels)
        + [pltpu.VMEM((sectors, cells, pixels), BF16)]
        + [pltpu.VMEM(a.shape, a.dtype) for a in (contexts[0], depths[0], ids[0])]
        + [pltpu.SemaphoreType.DMA((3,))],
        compiler_params=pltpu.CompilerParams(vmem_limit_bytes=VMEM_LIMIT),
        cost_estimate=pl.CostEstimate(
            flops=2 * sectors * len(slots) * cells * pixels * channels,
            bytes_accessed=2 * len(slots) * cells * channels,
            transcendentals=0,
        ),
        name="pool",
    )(place, *[a for args in zip(contexts, depths, ids) for a in args])


def pool_matrix(place, depths, ids, slots, piece_rows, chunk_order):
    bins, pixels = depths[0].shape
    sectors = len(depths)
    cells = piece_rows * GRID
    vmem = pl.BlockSpec(memory_space=pltpu.VMEM)
    return pl.pallas_call(
        functools.partial(
            match_kernel, slots=slots, piece_rows=piece_rows, chunk_order=chunk_order
        ),
        out_shape=jax.ShapeDtypeStruct((sectors, len(slots) * cells, pixels), BF16),
        in_specs=[pl.BlockSpec(memory_space=pltpu.SMEM)] + [vmem] * (2 * sectors),
        out_specs=vmem,
        scratch_shapes=hot_scratch(sectors, bins, pixels),
        compiler_params=pltpu.CompilerParams(vmem_limit_bytes=VMEM_LIMIT),
        cost_estimate=pl.CostEstimate(
            flops=2 * sectors * len(slots) * cells * pixels * bins,
            bytes_accessed=2 * len(slots) * cells * pixels,
            transcendentals=0,
        ),
        name="pool_matrix",
    )(place, *[a for args in zip(depths, ids) for a in args])


def pool_multiply(contexts, matrix, count):
    pixels, channels = contexts[0].shape
    cells = matrix.shape[1] // count
    vmem = pl.BlockSpec(memory_space=pltpu.VMEM)
    return pl.pallas_call(
        functools.partial(multiply_kernel, sectors=len(contexts)),
        out_shape=[jax.ShapeDtypeStruct((channels, cells), BF16)] * count,
        in_specs=[vmem] * (len(contexts) + 1),
        out_specs=[vmem] * count,
        scratch_shapes=[pltpu.VMEM((len(contexts), channels, pixels), BF16)],
        compiler_params=pltpu.CompilerParams(vmem_limit_bytes=VMEM_LIMIT),
        cost_estimate=pl.CostEstimate(
            flops=2 * matrix.size * channels,
            bytes_accessed=2 * matrix.size,
            transcendentals=0,
        ),
        name="pool_multiply",
    )(*contexts, matrix)


def prep_kernel(w_qkv, w_out, w_up, w_down, gain, embed, qkv_t, out_t, up_t, down_t, gains, embeds):
    _, channels, _ = w_qkv.shape
    hidden = w_up.shape[2]
    size = channels // HEADS
    row = lax.broadcasted_iota(jnp.int32, (channels, channels), 0)
    col = lax.broadcasted_iota(jnp.int32, (channels, channels), 1)
    order = (col == (row % HEADS) * size + row // HEADS).astype(F32).astype(BF16)
    same = (col == row).astype(F32).astype(BF16)

    def turned(left, right):
        return lax.dot_general(left, right, NT, preferred_element_type=F32).astype(BF16)

    def columns(values):
        return jnp.broadcast_to(values, (LANES, channels)).T

    for j in range(3):
        at = slice(j * channels, (j + 1) * channels)
        qkv_t[0, at, :] = turned(order, w_qkv[0, :, at])
    rows = jnp.dot(order, w_out[0], preferred_element_type=F32).astype(BF16)
    out_t[0] = turned(same, rows)
    for j in range(0, hidden, channels):
        at = slice(j, j + channels)
        up_t[0, at, :] = turned(same, w_up[0, :, at])
        down_t[0, :, at] = turned(same, w_down[0, at, :])
    for k in range(gain.shape[1]):
        gains[0, k] = columns(gain[0, k : k + 1, :])

    @pl.when(pl.program_id(0) == 0)
    def _():
        for f in range(embed.shape[0]):
            embeds[f] = columns(embed[f : f + 1, :].astype(F32))


def prep(w_qkv, w_out, w_up, w_down, norm_gain, time_embed):
    matrices = (w_qkv, w_out, w_up, w_down)
    channels = time_embed.shape[1]
    a_layer = lambda shape: pl.BlockSpec((1,) + shape[1:], lambda l: (l,) + (0,) * (len(shape) - 1))
    whole = lambda shape: pl.BlockSpec(shape, lambda l: (0,) * len(shape))
    gains = norm_gain.shape + (LANES,)
    embeds = time_embed.shape + (LANES,)
    turned = [(w.shape[0], w.shape[2], w.shape[1]) for w in matrices]
    return pl.pallas_call(
        prep_kernel,
        grid=(w_qkv.shape[0],),
        out_shape=[jax.ShapeDtypeStruct(shape, BF16) for shape in turned]
        + [jax.ShapeDtypeStruct(gains, F32), jax.ShapeDtypeStruct(embeds, F32)],
        in_specs=[a_layer(w.shape) for w in matrices]
        + [a_layer(norm_gain.shape), whole(time_embed.shape)],
        out_specs=[a_layer(shape) for shape in turned] + [a_layer(gains), whole(embeds)],
        compiler_params=pltpu.CompilerParams(
            dimension_semantics=("arbitrary",), vmem_limit_bytes=VMEM_LIMIT
        ),
        cost_estimate=pl.CostEstimate(
            flops=2 * channels * sum(w.size for w in matrices),
            bytes_accessed=4 * sum(w.size for w in matrices),
            transcendentals=0,
        ),
        name="prep",
    )(*matrices, norm_gain, time_embed)


def normed_tile(stream, gain):
    mean = jnp.mean(stream * stream, axis=0, keepdims=True)
    scale = lax.rsqrt(mean + 1e-05)
    lanes = stream.shape[1]
    gains = jnp.concatenate([gain] * (lanes // LANES), axis=1)
    return (stream * scale * gains).astype(BF16)


def gelu(values):
    root = (2.0 / math.pi) ** 0.5
    values = values.astype(BF16)
    half = 0.5 * values
    return half + half * jnp.tanh(values * (root + (root * 0.044715) * (values * values)))


def query_groups(frames, most):
    groups, group, pairs = [], [], 0
    for f in range(frames):
        if group and pairs + f + 1 > most:
            groups.append(group)
            group, pairs = [], 0
        group.append(f)
        pairs += f + 1
    return groups + [group]


def attention(qkv, mixed, frames, cells, channels):
    size = channels // HEADS
    for group in query_groups(frames, 40):
        last = group[-1]
        for lane in range(0, cells, LANES):
            pairs = [(f, g) for f in group for g in range(f + 1)]

            def at(f):
                return slice(f * cells + lane, f * cells + lane + LANES)

            def score_step(d, sums):
                row = pl.multiple_of(d * HEADS, HEADS)
                query = {f: qkv[pl.ds(row, HEADS), at(f)] for f in group}
                keys = [qkv[pl.ds(channels + row, HEADS), at(g)] for g in range(last + 1)]
                return tuple(s + query[f] * keys[g] for s, (f, g) in zip(sums, pairs))

            zeros = tuple(jnp.zeros((HEADS, LANES), F32) for _ in pairs)
            scores = dict(zip(pairs, lax.fori_loop(0, size, score_step, zeros, unroll=4)))
            weights = {}
            for f in group:
                row = [scores[f, g] for g in range(f + 1)]
                largest = functools.reduce(jnp.maximum, row)
                raised = [jnp.exp((s - largest) * size ** (-0.5)) for s in row]
                share = 1.0 / functools.reduce(jnp.add, raised)
                for g in range(f + 1):
                    weights[f, g] = (raised[g] * share).astype(BF16).astype(F32)

            def mix_step(step, carry):
                parts = {f: [] for f in group}
                for half in range(2):
                    row = pl.multiple_of(2 * channels + (2 * step + half) * HEADS, HEADS)
                    values = [qkv[pl.ds(row, HEADS), at(g)] for g in range(last + 1)]
                    for f in group:
                        terms = [carry[pairs.index((f, g))] * values[g] for g in range(f + 1)]
                        parts[f].append(functools.reduce(jnp.add, terms))
                low = pl.multiple_of(step * 2 * HEADS, 2 * HEADS)
                for f in group:
                    mixed[pl.ds(low, 2 * HEADS), at(f)] = jnp.concatenate(
                        parts[f], axis=0
                    ).astype(BF16)
                return carry

            lax.fori_loop(
                0, size // 2, mix_step, tuple(weights[pair] for pair in pairs), unroll=2
            )


def encode_kernel(place, *refs, slots, chunk, cells, valid, last, tile):
    *refs, stream, qkv, mixed = refs
    tokens, refs = refs[:slots], refs[slots:]
    embed, gains, qkv_t, out_t, up_t, down_t, *outs = refs
    half = slots // 2
    layers, _, channels = qkv_t.shape
    lanes = slots * cells
    for k in range(slots):
        frame = place[0] ^ k
        for lane in range(0, cells, LANES):
            at = pl.ds(pl.multiple_of(frame * cells + lane, LANES), LANES)
            low = chunk * cells + lane
            stream[:, at] = tokens[k][:, low : low + LANES].astype(F32) + embed[frame]

    def layer(l, _):
        def project(t, _):
            at = pl.ds(pl.multiple_of(t * tile, tile), tile)
            normed = normed_tile(stream[:, at], gains[l, 0])
            out = jnp.dot(qkv_t[l], normed, preferred_element_type=F32)
            qkv[:, at] = out.astype(BF16).astype(F32)
            return 0

        lax.fori_loop(0, lanes // tile, project, 0, unroll=2)
        attention(qkv, mixed, slots, cells, channels)

        def feed(t, _):
            at = pl.ds(pl.multiple_of(t * tile, tile), tile)
            current = stream[:, at] + jnp.dot(
                out_t[l], mixed[:, at], preferred_element_type=F32
            )
            normed = normed_tile(current, gains[l, 1])
            up = jnp.dot(up_t[l], normed, preferred_element_type=F32)
            hidden = gelu(up)
            stream[:, at] = current + jnp.dot(down_t[l], hidden, preferred_element_type=F32)
            return 0

        lax.fori_loop(0, lanes // tile, feed, 0, unroll=2)
        return 0

    lax.fori_loop(0, layers, layer, 0)
    earlier, outs = outs[:chunk] if last else [], outs[chunk:] if last else outs
    for k in range(slots):
        at = pl.ds(pl.multiple_of((place[0] ^ k) * cells, LANES), cells)
        done = stream[:, at].T.astype(BF16)[:valid]
        if not last:
            outs[k // half][k % half] = done
        elif k >= half:
            outs[k][...] = done
        else:
            for c, before in enumerate(earlier):
                outs[k][c * valid : (c + 1) * valid] = before[k]
            outs[k][chunk * valid : (chunk + 1) * valid] = done


def encode(place, tokens, weights, gains, embed, earlier, chunk, chunks):
    slots = len(tokens)
    half = slots // 2
    channels, piece_cells = tokens[0].shape
    valid = piece_cells // chunks
    spare = -valid % LANES
    if spare:
        tokens = [jnp.pad(t, ((0, 0), (0, spare))) for t in tokens]
    cells = valid + spare
    layers, hidden = weights[2].shape[:2]
    lanes = slots * cells
    last = chunk == chunks - 1
    if last:
        shapes = [(chunks * valid, channels)] * half + [(valid, channels)] * half
    else:
        shapes = [(half, valid, channels)] * 2
    vmem = pl.BlockSpec(memory_space=pltpu.VMEM)
    operands = [*tokens, embed, gains, *weights, *(earlier if last else [])]
    return pl.pallas_call(
        functools.partial(
            encode_kernel,
            slots=slots,
            chunk=chunk,
            cells=cells,
            valid=valid,
            last=last,
            tile=min(lanes, 512),
        ),
        out_shape=[jax.ShapeDtypeStruct(shape, BF16) for shape in shapes],
        in_specs=[pl.BlockSpec(memory_space=pltpu.SMEM)] + [vmem] * len(operands),
        out_specs=[vmem] * len(shapes),
        scratch_shapes=[
            pltpu.VMEM((channels, lanes), F32),
            pltpu.VMEM((3 * channels, lanes), F32),
            pltpu.VMEM((channels, lanes), BF16),
        ],
        compiler_params=pltpu.CompilerParams(vmem_limit_bytes=VMEM_LIMIT),
        cost_estimate=pl.CostEstimate(
            flops=2 * layers * lanes * channels * (4 * channels + 2 * hidden),
            bytes_accessed=4 * lanes * channels,
            transcendentals=layers * lanes * hidden,
        ),
        name="encode",
    )(place, *operands)


def edge_kernel(place, *refs, slots, rows, single):
    parts, outs = refs[:slots], refs[slots:]
    for k in range(slots):
        piece = place[0] ^ k
        is_head, is_tail = piece == 0, piece == slots - 1
        if single:
            is_head = jnp.logical_and(is_head, place[1] != 0)
            is_tail = jnp.logical_and(is_tail, place[1] == 0)

        @pl.when(is_head)
        def _():
            outs[0][...] = parts[k][0:GRID]

        @pl.when(is_tail)
        def _():
            outs[-1][...] = parts[k][rows - GRID : rows]


def edges(place, parts, rows, single):
    channels = parts[0].shape[1]
    vmem = pl.BlockSpec(memory_space=pltpu.VMEM)
    count = 1 if single else 2
    return pl.pallas_call(
        functools.partial(edge_kernel, slots=len(parts), rows=rows, single=single),
        out_shape=[jax.ShapeDtypeStruct((GRID, channels), BF16)] * count,
        in_specs=[pl.BlockSpec(memory_space=pltpu.SMEM)] + [vmem] * len(parts),
        out_specs=[vmem] * count,
        compiler_params=pltpu.CompilerParams(vmem_limit_bytes=VMEM_LIMIT),
        name="edges",
    )(place, *parts)


def conv_kernel(place, top, bottom, *refs, layout, chunks, piece_rows, bands, block):
    *parts, weight, out_ref, rows = refs
    slots = len(layout)
    total = slots * piece_rows
    inside = (place[1] > 0, place[1] < (bands - 1) * total)
    for edge, has, low in ((top, inside[0], 0), (bottom, inside[1], (total + 1) * GRID)):
        keep = jnp.full(edge.shape, has.astype(jnp.int32), jnp.int32) > 0
        rows[low : low + GRID] = jnp.where(keep, edge[...].astype(F32), 0.0).astype(BF16)
    for k in range(slots):
        base = (1 + (place[0] ^ k) * piece_rows) * GRID
        for c, chunk in enumerate(chunks):
            source, start = layout[k][c]
            for i, row in enumerate(chunk):
                low = pl.multiple_of(base + row * GRID, GRID)
                first = start + i * GRID
                rows[pl.ds(low, GRID)] = parts[source][first : first + GRID]

    cells = block * GRID
    column = lax.broadcasted_iota(jnp.int32, (cells, 1), 0) % GRID

    def one_block(n, _):
        def taps(j):
            sums = None
            for i in range(3):
                at = pl.ds(pl.multiple_of((n * block + i) * GRID, GRID), cells)
                product = jnp.dot(rows[at], weight[i, j], preferred_element_type=F32)
                sums = product if sums is None else sums + product
            return sums

        at = pl.ds(pl.multiple_of((n * block + 1) * GRID, GRID), cells)
        summed = rows[at].astype(F32) + taps(1)
        summed = summed + jnp.where(column == 0, 0.0, pltpu.roll(taps(0), 1, 0))
        summed = summed + jnp.where(column == GRID - 1, 0.0, pltpu.roll(taps(2), cells - 1, 0))
        out_ref[pl.ds(pl.multiple_of(n * cells, cells), cells)] = summed.astype(BF16)
        return 0

    lax.fori_loop(0, total // block, one_block, 0)


def convolve(place, top, bottom, parts, weight, layout, chunks, bands):
    channels = weight.shape[-1]
    piece_rows = sum(len(chunk) for chunk in chunks)
    total = len(layout) * piece_rows
    vmem = pl.BlockSpec(memory_space=pltpu.VMEM)
    return pl.pallas_call(
        functools.partial(
            conv_kernel,
            layout=layout,
            chunks=chunks,
            piece_rows=piece_rows,
            bands=bands,
            block=math.gcd(total, 8),
        ),
        out_shape=jax.ShapeDtypeStruct((total * GRID, channels), BF16),
        in_specs=[pl.BlockSpec(memory_space=pltpu.SMEM)] + [vmem] * (len(parts) + 3),
        out_specs=vmem,
        scratch_shapes=[pltpu.VMEM(((total + 2) * GRID, channels), BF16)],
        compiler_params=pltpu.CompilerParams(vmem_limit_bytes=VMEM_LIMIT),
        cost_estimate=pl.CostEstimate(
            flops=2 * total * GRID * weight.size,
            bytes_accessed=4 * total * GRID * channels,
            transcendentals=0,
        ),
        name="convolve",
    )(place, top, bottom, *parts, weight)


def row_chunks(piece_rows):
    if piece_rows % 4:
        return (tuple(range(piece_rows)),)
    quarter = piece_rows // 4
    inner = tuple(range(quarter, 3 * quarter))
    outer = tuple(range(quarter)) + tuple(range(3 * quarter, piece_rows))
    return (outer, inner)


def body(
    context, depth_weight, cell_ids, time_embed, norm_gain, w_qkv, w_out, w_up, w_down, conv_weight
):
    sectors = lax.axis_size("sector")
    slots = lax.axis_size("tm")
    half = slots // 2
    if context.shape[0] != 1 or slots & (slots - 1):
        raise ValueError("unsupported mesh")
    band_rows = GRID // sectors
    piece_rows = band_rows // slots
    chunks = row_chunks(piece_rows)
    valid = piece_rows * GRID // len(chunks)
    band = lax.axis_index("sector").astype(jnp.int32)
    place = jnp.stack([lax.axis_index("tm").astype(jnp.int32), band * band_rows])

    def from_others(value):
        values = [value]
        for shift in range(1, sectors):
            ring = [(i, (i + shift) % sectors) for i in range(sectors)]
            values.append(lax.ppermute(value, "sector", ring))
        return values

    def swap(value, k):
        if k == 0:
            return value
        return lax.ppermute(value, "tm", [(i, i ^ k) for i in range(slots)])

    order = (piece_rows, sum(chunks, ()))
    near = tuple(range(half))
    depth = swap(depth_weight[0, 0], half)
    features = swap(context[0, 0], half)
    contexts = from_others(context[0, 0])
    depths = from_others(depth_weight[0, 0])
    ids = from_others(cell_ids[0])
    depths_partner = from_others(depth)
    own = pool(place, contexts, depths, ids, near, *order)
    tokens = [swap(own[k], k) for k in near]
    matrix = pool_matrix(place, depths_partner, ids, near, *order)
    contexts = from_others(features)
    partner = pool_multiply(contexts, matrix, half)
    tokens += [swap(partner[k], k) for k in near]
    *weights, gains, embed = prep(w_qkv, w_out, w_up, w_down, norm_gain, time_embed)

    earlier, crossed = [], []
    for c in range(len(chunks) - 1):
        near_part, far_part = encode(place, tokens, weights, gains, embed, [], c, len(chunks))
        earlier.append(near_part)
        crossed.append(swap(far_part, half))
    outs = encode(
        place, tokens, weights, gains, embed, earlier, len(chunks) - 1, len(chunks)
    )
    parts, layout = [], [[None] * len(chunks) for _ in range(slots)]

    for k in range(half, slots):
        parts.append(swap(outs[k], k))
        layout[k][-1] = (len(parts) - 1, 0)
    for k in near:
        parts.append(swap(outs[k], k))
        for c in range(len(chunks)):
            layout[k][c] = (len(parts) - 1, c * valid)
    for c, received in enumerate(crossed):
        for k in near:
            parts.append(swap(received[k], k))
            layout[half + k][c] = (len(parts) - 1, 0)

    first = [parts[layout[k][0][0]] for k in range(slots)]
    up = [(i, i + 1) for i in range(sectors - 1)]
    down = [(i + 1, i) for i in range(sectors - 1)]
    if sectors == 2:
        (edge,) = edges(place, first, valid, True)
        top = bottom = lax.ppermute(edge, "sector", up + down)
    else:
        head, tail = edges(place, first, valid, False)
        top, bottom = lax.ppermute(tail, "sector", up), lax.ppermute(head, "sector", down)
    out = convolve(place, top, bottom, parts, conv_weight, layout, chunks, sectors)
    return out.reshape(1, band_rows, GRID, -1)


def solution(mesh):
    return jax.shard_map(
        body,
        mesh=mesh,
        in_specs=(
            P(("groups", "tm"), "sector", None, None),
            P(("groups", "tm"), "sector", None, None),
            P("sector", None, None),
            P(),
            P(),
            P(),
            P(),
            P(),
            P(),
            P(),
        ),
        out_specs=P(("groups", "tm"), "sector", None, None),
        check_vma=False,
    )
```

```python
import functools
import math

import jax
import jax.numpy as jnp
from jax import lax
from jax.experimental import pallas as pl
from jax.experimental.pallas import tpu as pltpu
from jax.sharding import PartitionSpec as P


HEADS = 8
GRID = 64
LANES = 128
TILE_LANES = 256
SUBLANES = 8
MERGED = 2
VMEM_LIMIT = 24 << 20
F32 = jnp.float32
BF16 = jnp.bfloat16
NT = (((1,), (1,)), ((), ()))


def mark(weights, ids, col_hot, row_id):
    bins, pixels = weights[0].shape
    wide = (SUBLANES, pixels)
    column = lax.broadcasted_iota(jnp.int32, wide, 0).astype(F32).astype(BF16)
    tiles = [slice(low, low + SUBLANES) for low in range(0, GRID, SUBLANES)]
    count = math.gcd(bins, MERGED)

    def spread(line):
        return jnp.broadcast_to(line, wide).astype(BF16)

    for s in range(len(weights)):

        def merge(n, _):
            row, hot = [], []
            for k in range(count):
                d = n * count + k
                cell = ids[s][pl.ds(d, 1), :]
                line = cell >> (GRID.bit_length() - 1)
                row.append(spread(line.astype(F32)))
                col = spread((cell & (GRID - 1)).astype(F32))
                value = spread(weights[s][pl.ds(d, 1), :])
                hot.append((col, value))
            for at in tiles:
                parts = []
                for col, value in hot:
                    hit = column + at.start == col
                    parts.append(jnp.where(hit, value, jnp.zeros_like(value)))
                for k in range(count):
                    for later in range(k + 1, count):
                        more = jnp.where(row[later] == row[k], parts[later], jnp.zeros(wide, BF16))
                        parts[k] = parts[k] + more
                    col_hot[s, n * count + k, at] = parts[k]
            for k in range(count):
                lone = row[k]
                for earlier in range(k):
                    lone = jnp.where(row[earlier] == row[k], jnp.full(wide, -1.0, BF16), lone)
                row_id[s, n * count + k] = lone
            return 0

        lax.fori_loop(0, bins // count, merge, 0)


def match(place, slot, matrix, base, col_hot, row_id, piece_rows, chunk_order):
    sectors, bins, _, pixels = col_hot.shape
    blocks = pixels // TILE_LANES
    shape = (SUBLANES, TILE_LANES)
    piece = place[0] ^ slot
    for first in range(0, piece_rows, 2):
        targets = []
        for row in chunk_order[first : first + 2]:
            target = (place[1] + piece * piece_rows + row).astype(F32)
            targets.append(jnp.full(shape, target, F32).astype(BF16))

        def step(n, _):
            s = n // blocks
            at = pl.ds(pl.multiple_of((n % blocks) * TILE_LANES, TILE_LANES), TILE_LANES)
            sums = [[jnp.zeros(shape, BF16)] * (GRID // SUBLANES) for _ in targets]
            count = math.gcd(bins, MERGED)
            for low in range(0, bins, count):
                group = range(low, low + count)
                hits = [[row_id[s, d, :, at] == target for target in targets] for d in group]
                for j in range(GRID // SUBLANES):
                    tile = slice(j * SUBLANES, (j + 1) * SUBLANES)
                    found = [jnp.zeros(shape, BF16) for _ in targets]
                    for d, hit in zip(group, hits):
                        part = col_hot[s, d, tile, at]
                        found = [jnp.where(h, part, f) for h, f in zip(hit, found)]
                    for k in range(len(targets)):
                        sums[k][j] = sums[k][j] + found[k]
            for k in range(len(targets)):
                for j in range(GRID // SUBLANES):
                    low = base + (first + k) * GRID + j * SUBLANES
                    matrix[s, low : low + SUBLANES, at] = sums[k][j]
            return 0

        lax.fori_loop(0, sectors * blocks, step, 0)


def multiply(context_t, matrix, low, cells):
    total = None
    for s in range(matrix.shape[0]):
        rows = matrix[s, low : low + cells]
        part = lax.dot_general(context_t[s], rows, NT, preferred_element_type=F32)
        part = part.astype(BF16).astype(F32)
        total = part if total is None else total + part
    return total.astype(BF16)


def pool_kernel(place, *refs, slots, piece_rows, chunk_order):
    *refs, context_t, col_hot, row_id, matrix, context, weight, ids, arrived = refs
    out_refs, refs = refs[-len(slots) :], refs[: -len(slots)]
    held = (context, weight, ids)
    copies = [pltpu.make_async_copy(refs[n], held[n], arrived.at[n]) for n in range(3)]
    for copy in copies:
        copy.start()
    for copy in copies:
        copy.wait()
    refs = held + tuple(refs[3:])
    mark(refs[1::3], refs[2::3], col_hot, row_id)
    for s, context in enumerate(refs[0::3]):
        context_t[s] = context[...].astype(F32).T.astype(BF16)
    for slot, out_ref in zip(slots, out_refs):
        match(place, slot, matrix, 0, col_hot, row_id, piece_rows, chunk_order)
        out_ref[...] = multiply(context_t, matrix, 0, matrix.shape[1])


def match_kernel(place, *refs, slots, piece_rows, chunk_order):
    *refs, matrix, col_hot, row_id = refs
    mark(refs[0::2], refs[1::2], col_hot, row_id)
    cells = piece_rows * GRID
    for n, slot in enumerate(slots):
        match(place, slot, matrix, n * cells, col_hot, row_id, piece_rows, chunk_order)


def multiply_kernel(*refs, sectors, chunks):
    contexts, matrix = refs[:sectors], refs[sectors]
    out_refs, context_t = refs[sectors + 1 : -1], refs[-1]
    for s in range(sectors):
        context_t[s] = contexts[s][...].astype(F32).T.astype(BF16)
    valid = matrix.shape[1] // len(out_refs)
    cells = valid * chunks
    for n in range(len(out_refs) // chunks):
        done = multiply(context_t, matrix, n * cells, cells)
        for c in range(chunks):
            out_refs[n * chunks + c][...] = done[:, c * valid : (c + 1) * valid]


def hot_scratch(sectors, bins, pixels):
    return [
        pltpu.VMEM((sectors, bins, GRID, pixels), BF16),
        pltpu.VMEM((sectors, bins, SUBLANES, pixels), BF16),
    ]


def pool(place, contexts, depths, ids, slots, piece_rows, chunk_order):
    pixels, channels = contexts[0].shape
    bins = depths[0].shape[0]
    sectors = len(contexts)
    cells = piece_rows * GRID
    vmem = pl.BlockSpec(memory_space=pltpu.VMEM)
    return pl.pallas_call(
        functools.partial(
            pool_kernel, slots=slots, piece_rows=piece_rows, chunk_order=chunk_order
        ),
        out_shape=[jax.ShapeDtypeStruct((channels, cells), BF16)] * len(slots),
        in_specs=[pl.BlockSpec(memory_space=pltpu.SMEM)]
        + [pl.BlockSpec(memory_space=pltpu.HBM)] * 3
        + [vmem] * (3 * sectors - 3),
        out_specs=[vmem] * len(slots),
        scratch_shapes=[pltpu.VMEM((sectors, channels, pixels), BF16)]
        + hot_scratch(sectors, bins, pixels)
        + [pltpu.VMEM((sectors, cells, pixels), BF16)]
        + [pltpu.VMEM(a.shape, a.dtype) for a in (contexts[0], depths[0], ids[0])]
        + [pltpu.SemaphoreType.DMA((3,))],
        compiler_params=pltpu.CompilerParams(vmem_limit_bytes=VMEM_LIMIT),
        cost_estimate=pl.CostEstimate(
            flops=2 * sectors * len(slots) * cells * pixels * channels,
            bytes_accessed=2 * len(slots) * cells * channels,
            transcendentals=0,
        ),
        name="pool",
    )(place, *[a for args in zip(contexts, depths, ids) for a in args])


def pool_matrix(place, depths, ids, slots, piece_rows, chunk_order):
    bins, pixels = depths[0].shape
    sectors = len(depths)
    cells = piece_rows * GRID
    vmem = pl.BlockSpec(memory_space=pltpu.VMEM)
    return pl.pallas_call(
        functools.partial(
            match_kernel, slots=slots, piece_rows=piece_rows, chunk_order=chunk_order
        ),
        out_shape=jax.ShapeDtypeStruct((sectors, len(slots) * cells, pixels), BF16),
        in_specs=[pl.BlockSpec(memory_space=pltpu.SMEM)] + [vmem] * (2 * sectors),
        out_specs=vmem,
        scratch_shapes=hot_scratch(sectors, bins, pixels),
        compiler_params=pltpu.CompilerParams(vmem_limit_bytes=VMEM_LIMIT),
        cost_estimate=pl.CostEstimate(
            flops=2 * sectors * len(slots) * cells * pixels * bins,
            bytes_accessed=2 * len(slots) * cells * pixels,
            transcendentals=0,
        ),
        name="pool_matrix",
    )(place, *[a for args in zip(depths, ids) for a in args])


def pool_multiply(contexts, matrix, slots, chunks):
    pixels, channels = contexts[0].shape
    cells = matrix.shape[1] // slots
    valid = cells // chunks
    vmem = pl.BlockSpec(memory_space=pltpu.VMEM)
    outs = pl.pallas_call(
        functools.partial(multiply_kernel, sectors=len(contexts), chunks=chunks),
        out_shape=[jax.ShapeDtypeStruct((channels, valid), BF16)] * (slots * chunks),
        in_specs=[vmem] * (len(contexts) + 1),
        out_specs=[vmem] * (slots * chunks),
        scratch_shapes=[pltpu.VMEM((len(contexts), channels, pixels), BF16)],
        compiler_params=pltpu.CompilerParams(vmem_limit_bytes=VMEM_LIMIT),
        cost_estimate=pl.CostEstimate(
            flops=2 * matrix.size * channels,
            bytes_accessed=2 * matrix.size,
            transcendentals=0,
        ),
        name="pool_multiply",
    )(*contexts, matrix)
    return [outs[n * chunks : (n + 1) * chunks] for n in range(slots)]


def prep_kernel(w_qkv, w_out, w_up, w_down, gain, embed, qkv_t, out_t, up_t, down_t, gains, embeds):
    _, channels, _ = w_qkv.shape
    hidden = w_up.shape[2]
    size = channels // HEADS
    row = lax.broadcasted_iota(jnp.int32, (channels, channels), 0)
    col = lax.broadcasted_iota(jnp.int32, (channels, channels), 1)
    order = (col == (row % HEADS) * size + row // HEADS).astype(F32).astype(BF16)
    same = (col == row).astype(F32).astype(BF16)

    def turned(left, right):
        return lax.dot_general(left, right, NT, preferred_element_type=F32).astype(BF16)

    def columns(values):
        return jnp.broadcast_to(values, (LANES, channels)).T

    for j in range(3):
        at = slice(j * channels, (j + 1) * channels)
        qkv_t[0, at, :] = turned(order, w_qkv[0, :, at])
    rows = jnp.dot(order, w_out[0], preferred_element_type=F32).astype(BF16)
    out_t[0] = turned(same, rows)
    for j in range(0, hidden, channels):
        at = slice(j, j + channels)
        up_t[0, at, :] = turned(same, w_up[0, :, at])
        down_t[0, :, at] = turned(same, w_down[0, at, :])
    for k in range(gain.shape[1]):
        gains[0, k] = columns(gain[0, k : k + 1, :])

    @pl.when(pl.program_id(0) == 0)
    def _():
        for f in range(embed.shape[0]):
            embeds[f] = columns(embed[f : f + 1, :].astype(F32))


def prep(w_qkv, w_out, w_up, w_down, norm_gain, time_embed):
    matrices = (w_qkv, w_out, w_up, w_down)
    channels = time_embed.shape[1]
    a_layer = lambda shape: pl.BlockSpec((1,) + shape[1:], lambda l: (l,) + (0,) * (len(shape) - 1))
    whole = lambda shape: pl.BlockSpec(shape, lambda l: (0,) * len(shape))
    gains = norm_gain.shape + (LANES,)
    embeds = time_embed.shape + (LANES,)
    turned = [(w.shape[0], w.shape[2], w.shape[1]) for w in matrices]
    return pl.pallas_call(
        prep_kernel,
        grid=(w_qkv.shape[0],),
        out_shape=[jax.ShapeDtypeStruct(shape, BF16) for shape in turned]
        + [jax.ShapeDtypeStruct(gains, F32), jax.ShapeDtypeStruct(embeds, F32)],
        in_specs=[a_layer(w.shape) for w in matrices]
        + [a_layer(norm_gain.shape), whole(time_embed.shape)],
        out_specs=[a_layer(shape) for shape in turned] + [a_layer(gains), whole(embeds)],
        compiler_params=pltpu.CompilerParams(
            dimension_semantics=("arbitrary",), vmem_limit_bytes=VMEM_LIMIT
        ),
        cost_estimate=pl.CostEstimate(
            flops=2 * channels * sum(w.size for w in matrices),
            bytes_accessed=4 * sum(w.size for w in matrices),
            transcendentals=0,
        ),
        name="prep",
    )(*matrices, norm_gain, time_embed)


def normed_tile(stream, gain):
    mean = jnp.mean(stream * stream, axis=0, keepdims=True)
    scale = lax.rsqrt(mean + 1e-05)
    lanes = stream.shape[1]
    gains = jnp.concatenate([gain] * (lanes // LANES), axis=1)
    return (stream * scale * gains).astype(BF16)


def gelu(values):
    root = (2.0 / math.pi) ** 0.5
    values = values.astype(BF16)
    half = 0.5 * values
    return half + half * jnp.tanh(values * (root + (root * 0.044715) * (values * values)))


def query_groups(frames, most):
    groups, group, pairs = [], [], 0
    for f in range(frames):
        if group and pairs + f + 1 > most:
            groups.append(group)
            group, pairs = [], 0
        group.append(f)
        pairs += f + 1
    return groups + [group]


def attention(qkv, mixed, frames, cells, channels):
    size = channels // HEADS
    for group in query_groups(frames, 40):
        last = group[-1]
        for lane in range(0, cells, LANES):
            pairs = [(f, g) for f in group for g in range(f + 1)]

            def at(f):
                return slice(f * cells + lane, f * cells + lane + LANES)

            def score_step(d, sums):
                row = pl.multiple_of(d * HEADS, HEADS)
                query = {f: qkv[pl.ds(row, HEADS), at(f)] for f in group}
                keys = [qkv[pl.ds(channels + row, HEADS), at(g)] for g in range(last + 1)]
                return tuple(s + query[f] * keys[g] for s, (f, g) in zip(sums, pairs))

            zeros = tuple(jnp.zeros((HEADS, LANES), F32) for _ in pairs)
            scores = dict(zip(pairs, lax.fori_loop(0, size, score_step, zeros, unroll=4)))
            weights = {}
            for f in group:
                row = [scores[f, g] for g in range(f + 1)]
                largest = functools.reduce(jnp.maximum, row)
                raised = [jnp.exp((s - largest) * size ** (-0.5)) for s in row]
                share = 1.0 / functools.reduce(jnp.add, raised)
                for g in range(f + 1):
                    weights[f, g] = (raised[g] * share).astype(BF16).astype(F32)

            def mix_step(step, carry):
                parts = {f: [] for f in group}
                for half in range(2):
                    row = pl.multiple_of(2 * channels + (2 * step + half) * HEADS, HEADS)
                    values = [qkv[pl.ds(row, HEADS), at(g)] for g in range(last + 1)]
                    for f in group:
                        terms = [carry[pairs.index((f, g))] * values[g] for g in range(f + 1)]
                        parts[f].append(functools.reduce(jnp.add, terms))
                low = pl.multiple_of(step * 2 * HEADS, 2 * HEADS)
                for f in group:
                    mixed[pl.ds(low, 2 * HEADS), at(f)] = jnp.concatenate(
                        parts[f], axis=0
                    ).astype(BF16)
                return carry

            lax.fori_loop(
                0, size // 2, mix_step, tuple(weights[pair] for pair in pairs), unroll=2
            )


def encode_kernel(place, *refs, slots, chunk, cells, valid, last, tile):
    *refs, stream, qkv, mixed = refs
    tokens, refs = refs[:slots], refs[slots:]
    embed, gains, qkv_t, out_t, up_t, down_t, *outs = refs
    half = slots // 2
    layers, _, channels = qkv_t.shape
    lanes = slots * cells
    for k in range(slots):
        frame = place[0] ^ k
        for lane in range(0, cells, LANES):
            at = pl.ds(pl.multiple_of(frame * cells + lane, LANES), LANES)
            low = lane + (chunk * cells if tokens[k].shape[1] > cells else 0)
            stream[:, at] = tokens[k][:, low : low + LANES].astype(F32) + embed[frame]

    def layer(l, _):
        def project(t, _):
            at = pl.ds(pl.multiple_of(t * tile, tile), tile)
            normed = normed_tile(stream[:, at], gains[l, 0])
            out = jnp.dot(qkv_t[l], normed, preferred_element_type=F32)
            qkv[:, at] = out.astype(BF16).astype(F32)
            return 0

        lax.fori_loop(0, lanes // tile, project, 0, unroll=2)
        attention(qkv, mixed, slots, cells, channels)

        def feed(t, _):
            at = pl.ds(pl.multiple_of(t * tile, tile), tile)
            current = stream[:, at] + jnp.dot(
                out_t[l], mixed[:, at], preferred_element_type=F32
            )
            normed = normed_tile(current, gains[l, 1])
            up = jnp.dot(up_t[l], normed, preferred_element_type=F32)
            hidden = gelu(up)
            stream[:, at] = current + jnp.dot(down_t[l], hidden, preferred_element_type=F32)
            return 0

        lax.fori_loop(0, lanes // tile, feed, 0, unroll=2)
        return 0

    lax.fori_loop(0, layers, layer, 0)
    earlier, outs = outs[:chunk] if last else [], outs[chunk:] if last else outs
    for k in range(slots):
        at = pl.ds(pl.multiple_of((place[0] ^ k) * cells, LANES), cells)
        done = stream[:, at].astype(BF16).T[:valid]
        if not last:
            outs[k // half][k % half] = done
        elif k >= half:
            outs[k][...] = done
        else:
            for c, before in enumerate(earlier):
                outs[k][c * valid : (c + 1) * valid] = before[k]
            outs[k][chunk * valid : (chunk + 1) * valid] = done


def encode(place, tokens, weights, gains, embed, earlier, chunk, chunks):
    slots = len(tokens)
    half = slots // 2
    channels, valid = tokens[-1].shape
    spare = -valid % LANES
    if spare:
        tokens = [jnp.pad(t, ((0, 0), (0, spare))) for t in tokens]
    cells = valid + spare
    layers, hidden = weights[2].shape[:2]
    lanes = slots * cells
    last = chunk == chunks - 1
    if last:
        shapes = [(chunks * valid, channels)] * half + [(valid, channels)] * half
    else:
        shapes = [(half, valid, channels)] * 2
    vmem = pl.BlockSpec(memory_space=pltpu.VMEM)
    operands = [*tokens, embed, gains, *weights, *(earlier if last else [])]
    return pl.pallas_call(
        functools.partial(
            encode_kernel,
            slots=slots,
            chunk=chunk,
            cells=cells,
            valid=valid,
            last=last,
            tile=min(lanes, 512),
        ),
        out_shape=[jax.ShapeDtypeStruct(shape, BF16) for shape in shapes],
        in_specs=[pl.BlockSpec(memory_space=pltpu.SMEM)] + [vmem] * len(operands),
        out_specs=[vmem] * len(shapes),
        scratch_shapes=[
            pltpu.VMEM((channels, lanes), F32),
            pltpu.VMEM((3 * channels, lanes), F32),
            pltpu.VMEM((channels, lanes), BF16),
        ],
        compiler_params=pltpu.CompilerParams(vmem_limit_bytes=VMEM_LIMIT),
        cost_estimate=pl.CostEstimate(
            flops=2 * layers * lanes * channels * (4 * channels + 2 * hidden),
            bytes_accessed=4 * lanes * channels,
            transcendentals=layers * lanes * hidden,
        ),
        name="encode",
    )(place, *operands)


def edge_kernel(place, *refs, slots, rows, single):
    parts, outs = refs[:slots], refs[slots:]
    for k in range(slots):
        piece = place[0] ^ k
        is_head, is_tail = piece == 0, piece == slots - 1
        if single:
            is_head = jnp.logical_and(is_head, place[1] != 0)
            is_tail = jnp.logical_and(is_tail, place[1] == 0)

        @pl.when(is_head)
        def _():
            outs[0][...] = parts[k][0:GRID]

        @pl.when(is_tail)
        def _():
            outs[-1][...] = parts[k][rows - GRID : rows]


def edges(place, parts, rows, single):
    channels = parts[0].shape[1]
    vmem = pl.BlockSpec(memory_space=pltpu.VMEM)
    count = 1 if single else 2
    return pl.pallas_call(
        functools.partial(edge_kernel, slots=len(parts), rows=rows, single=single),
        out_shape=[jax.ShapeDtypeStruct((GRID, channels), BF16)] * count,
        in_specs=[pl.BlockSpec(memory_space=pltpu.SMEM)] + [vmem] * len(parts),
        out_specs=[vmem] * count,
        compiler_params=pltpu.CompilerParams(vmem_limit_bytes=VMEM_LIMIT),
        name="edges",
    )(place, *parts)


def conv_kernel(place, top, bottom, *refs, layout, chunks, piece_rows, bands, block, part):
    *refs, out_ref, rows, outs, sent = refs
    if part == "rest":
        refs = refs[:-1]
    *parts, weight = refs
    slots = len(layout)
    half = slots // 2
    total = slots * piece_rows
    inside = (place[1] > 0, place[1] < (bands - 1) * total)
    for edge, has, low in ((top, inside[0], 0), (bottom, inside[1], (total + 1) * GRID)):
        keep = jnp.full(edge.shape, has.astype(jnp.int32), jnp.int32) > 0
        rows[low : low + GRID] = jnp.where(keep, edge[...].astype(F32), 0.0).astype(BF16)
    for k in range(slots):
        base = (1 + (place[0] ^ k) * piece_rows) * GRID
        for c, chunk in enumerate(chunks):
            if layout[k][c] is None:
                continue
            source, start = layout[k][c]
            for i, row in enumerate(chunk):
                low = pl.multiple_of(base + row * GRID, GRID)
                first = start + i * GRID
                rows[pl.ds(low, GRID)] = parts[source][first : first + GRID]

    cells = block * GRID
    column = lax.broadcasted_iota(jnp.int32, (cells, 1), 0) % GRID
    own = place[0] // half
    each = total // block // 2
    blocks = {"all": 2 * each, "inner": each - 2, "rest": each + 2}[part]

    def block_at(n):
        if part == "all":
            return n
        if part == "inner":
            return own * each + 1 + n
        end = own * each + jnp.where(n == each, 0, each - 1)
        return jnp.where(n < each, (1 - own) * each + n, end)

    def send(n):
        at = pl.ds(pl.multiple_of(block_at(n) * cells, cells), cells)
        here = pl.ds(pl.multiple_of(n * cells, cells), cells)
        return pltpu.make_async_copy(outs.at[here], out_ref.at[at], sent.at[n])

    def one_block(n, _):
        where = block_at(n)

        def taps(j):
            sums = None
            for i in range(3):
                at = pl.ds(pl.multiple_of((where * block + i) * GRID, GRID), cells)
                product = jnp.dot(rows[at], weight[i, j], preferred_element_type=F32)
                sums = product if sums is None else sums + product
            return sums

        at = pl.ds(pl.multiple_of((where * block + 1) * GRID, GRID), cells)
        summed = rows[at].astype(F32) + taps(1)
        summed = summed + jnp.where(column == 0, 0.0, pltpu.roll(taps(0), 1, 0))
        summed = summed + jnp.where(column == GRID - 1, 0.0, pltpu.roll(taps(2), cells - 1, 0))
        outs[pl.ds(pl.multiple_of(n * cells, cells), cells)] = summed.astype(BF16)
        send(n).start()
        return 0

    lax.fori_loop(0, blocks, one_block, 0)
    for n in range(blocks):
        send(n).wait()


def convolve(place, top, bottom, parts, weight, layout, chunks, bands, part, before=None):
    channels = weight.shape[-1]
    piece_rows = sum(len(chunk) for chunk in chunks)
    total = len(layout) * piece_rows
    block = math.gcd(total // 2, 4)
    each = total // block // 2
    done = {"all": 2 * each, "inner": each - 2, "rest": each + 2}[part] * block
    vmem = pl.BlockSpec(memory_space=pltpu.VMEM)
    hbm = pl.BlockSpec(memory_space=pltpu.HBM)
    operands = [place, top, bottom, *parts, weight]
    aliases = {}
    in_specs = [pl.BlockSpec(memory_space=pltpu.SMEM)] + [vmem] * (len(operands) - 1)
    if part == "rest":
        aliases = {len(operands): 0}
        operands.append(before)
        in_specs.append(hbm)
    return pl.pallas_call(
        functools.partial(
            conv_kernel,
            layout=layout,
            chunks=chunks,
            piece_rows=piece_rows,
            bands=bands,
            block=block,
            part=part,
        ),
        out_shape=jax.ShapeDtypeStruct((total * GRID, channels), BF16),
        in_specs=in_specs,
        out_specs=hbm,
        scratch_shapes=[
            pltpu.VMEM(((total + 2) * GRID, channels), BF16),
            pltpu.VMEM((done * GRID, channels), BF16),
            pltpu.SemaphoreType.DMA((done // block,)),
        ],
        input_output_aliases=aliases,
        compiler_params=pltpu.CompilerParams(vmem_limit_bytes=VMEM_LIMIT),
        cost_estimate=pl.CostEstimate(
            flops=2 * done * GRID * weight.size,
            bytes_accessed=4 * done * GRID * channels,
            transcendentals=0,
        ),
        name="convolve",
    )(*operands)


def row_chunks(piece_rows):
    if piece_rows % 4:
        return (tuple(range(piece_rows)),)
    quarter = piece_rows // 4
    inner = tuple(range(quarter, 3 * quarter))
    outer = tuple(range(quarter)) + tuple(range(3 * quarter, piece_rows))
    return (outer, inner)


def body(
    context, depth_weight, cell_ids, time_embed, norm_gain, w_qkv, w_out, w_up, w_down, conv_weight
):
    sectors = lax.axis_size("sector")
    slots = lax.axis_size("tm")
    half = slots // 2
    if context.shape[0] != 1 or slots & (slots - 1):
        raise ValueError("unsupported mesh")
    band_rows = GRID // sectors
    piece_rows = band_rows // slots
    chunks = row_chunks(piece_rows)
    valid = piece_rows * GRID // len(chunks)
    band = lax.axis_index("sector").astype(jnp.int32)
    place = jnp.stack([lax.axis_index("tm").astype(jnp.int32), band * band_rows])

    def from_others(value):
        values = [value]
        for shift in range(1, sectors):
            ring = [(i, (i + shift) % sectors) for i in range(sectors)]
            values.append(lax.ppermute(value, "sector", ring))
        return values

    def swap(value, k):
        if k == 0:
            return value
        return lax.ppermute(value, "tm", [(i, i ^ k) for i in range(slots)])

    order = (piece_rows, sum(chunks, ()))
    near = tuple(range(half))
    depth = swap(depth_weight[0, 0], half)
    features = swap(context[0, 0], half)
    contexts = from_others(context[0, 0])
    depths = from_others(depth_weight[0, 0])
    ids = from_others(cell_ids[0])
    depths_partner = from_others(depth)
    own = pool(place, contexts, depths, ids, near, *order)
    tokens = [swap(own[k], k) for k in near]
    matrix = pool_matrix(place, depths_partner, ids, near, *order)
    contexts = from_others(features)
    partner = pool_multiply(contexts, matrix, half, len(chunks))
    later_tokens = [[swap(partner[k][c], k) for k in near] for c in range(len(chunks))]
    *weights, gains, embed = prep(w_qkv, w_out, w_up, w_down, norm_gain, time_embed)

    earlier, crossed = [], []
    for c in range(len(chunks) - 1):
        slot_tokens = tokens + later_tokens[c]
        near_part, far_part = encode(
            place, slot_tokens, weights, gains, embed, [], c, len(chunks)
        )
        earlier.append(near_part)
        crossed.append(swap(far_part, half))
    slot_tokens = tokens + later_tokens[-1]
    outs = encode(
        place, slot_tokens, weights, gains, embed, earlier, len(chunks) - 1, len(chunks)
    )
    parts, layout = [], [[None] * len(chunks) for _ in range(slots)]
    for k in near:
        parts.append(swap(outs[k], k))
        for c in range(len(chunks)):
            layout[k][c] = (len(parts) - 1, c * valid)
    early_parts, early_layout = list(parts), [list(places) for places in layout]
    for c, received in enumerate(crossed):
        for k in near:
            parts.append(swap(received[k], k))
            layout[half + k][c] = (len(parts) - 1, 0)
    for k in range(half, slots):
        parts.append(swap(outs[k], k))
        layout[k][-1] = (len(parts) - 1, 0)

    first = [parts[layout[k][0][0]] for k in range(slots)]
    up = [(i, i + 1) for i in range(sectors - 1)]
    down = [(i + 1, i) for i in range(sectors - 1)]
    ends = edges(place, first, valid, sectors == 2)
    if sectors == 2:
        top = bottom = lax.ppermute(ends[0], "sector", up + down)
    else:
        head, tail = ends
        top, bottom = lax.ppermute(tail, "sector", up), lax.ppermute(head, "sector", down)
    ends = (conv_weight, layout, chunks, sectors)
    if len(chunks) > 1:
        nothing = jnp.zeros_like(top)
        inner = (conv_weight, early_layout, chunks, sectors)
        out = convolve(place, nothing, nothing, early_parts, *inner, "inner")
        out = convolve(place, top, bottom, parts, *ends, "rest", out)
    else:
        out = convolve(place, top, bottom, parts, *ends, "all")
    return out.reshape(1, band_rows, GRID, -1)


def solution(mesh):
    return jax.shard_map(
        body,
        mesh=mesh,
        in_specs=(
            P(("groups", "tm"), "sector", None, None),
            P(("groups", "tm"), "sector", None, None),
            P("sector", None, None),
            P(),
            P(),
            P(),
            P(),
            P(),
            P(),
            P(),
        ),
        out_specs=P(("groups", "tm"), "sector", None, None),
        check_vma=False,
    )
```
